256 devices in a mesh: pop: 4 (over x, y), chain: 64 (over z, core).
Axes of the slice: x: 2, y: 2, z: 32, core: 2. Of those that a mesh axis runs over, the one named last changes fastest.
The devices are a block of a 4x8x32 slice.
Arguments:
- cost: float32 [65536, 4096], P(('pop', 'chain')), parts along dimension 0, may hold values from 0 to 20
- marginals: float32 [65536], P(('pop', 'chain')), parts along dimension 0, may hold values from 0.125 to 6
- final_marginal: float32 [16384], P('pop'), parts along dimension 0, may hold values from 0.125 to 6
Outputs:
- log_scaling: float32 [65536], P(('pop', 'chain')), parts along dimension 0
The draws below stay inside these ranges and needn't reach their ends.
There are 4 independent parts, one for each index of `pop`. The reference program is written for one: setup_inputs(seed, part) draws one part's arguments, and reference() takes and returns one part's arrays. A program takes and returns all parts, laid end to end along the dimension named above; each array names one. Nothing has to cross between parts.
All inputs are finite; a program needn't handle non-finite values.
Results may differ from the reference program's by a relative error of at most 0.0001.
Values sent between devices are 32-bit elements; how exact they have to be, the bound alone decides.
A program may use at most 64 MiB of HBM per device.

```python
import math
import jax
import jax.numpy as jnp
from jax import lax

STATES = 4096
SWEEPS = 2
KERNELS = 4


def ramped_mass(key, entries):
    base_key = jax.random.fold_in(key, 11)
    baseline = jnp.exp(jax.random.uniform(base_key, (entries,), jnp.float32, math.log(0.25), math.log(4.0)))
    position = (jnp.arange(entries) % STATES).astype(jnp.float32)
    return baseline * (0.5 + position / STATES)


def draw_marginals(key, part):
    return ramped_mass(jax.random.fold_in(key, 3), KERNELS * STATES)


def draw_final_marginal(key, part):
    return ramped_mass(jax.random.fold_in(key, 5), STATES)


def draw_cost(key, part):
    row_total = KERNELS * STATES
    rough_key = jax.random.fold_in(key, 21)
    offset_key = jax.random.fold_in(key, 22)
    block_key = jax.random.fold_in(key, 23)
    rough_draw = jax.random.uniform(rough_key, (row_total, STATES), jnp.float32, 0.0, 1.0)
    offset_draw = jax.random.uniform(offset_key, (row_total, 1), jnp.float32, 0.0, 1.0)
    roughness = 12.0 * rough_draw
    row_offset = 4.0 * offset_draw
    block_draw = jax.random.uniform(block_key, (KERNELS, 4, 4), jnp.float32, 0.0, 1.0)
    diagonal_mask = jnp.eye(4, dtype=jnp.float32)
    block_cost = diagonal_mask * (0.5 * block_draw) + (1.0 - diagonal_mask) * (2.5 + block_draw)
    row_index = jnp.arange(row_total)
    kernel_index = row_index // STATES
    row_cluster = row_index % STATES * 4 // STATES
    column_cluster = jnp.arange(STATES) * 4 // STATES
    block_rows = block_cost[kernel_index, row_cluster]
    penalty = jnp.take(block_rows, column_cluster, axis=1)
    return jnp.clip(roughness + row_offset + penalty, 0.0, 20.0)


def setup_inputs(seed: int = 0, part: int = 0) -> dict:
    arg_keys = jax.random.split(jax.random.key(seed), 4)
    part_splits = jax.random.split(jax.random.fold_in(arg_keys[3], part), 4)
    cost = draw_cost(jax.random.fold_in(jax.random.fold_in(arg_keys[3], part), 71), part)
    marginals = draw_marginals(jax.random.fold_in(jax.random.fold_in(arg_keys[3], part), 71), part)
    final_marginal = draw_final_marginal(jax.random.fold_in(jax.random.fold_in(arg_keys[3], part), 71), part)
    return {"cost": cost, "marginals": marginals, "final_marginal": final_marginal}


entropic = 0.25


def reference(cost, marginals, final_marginal):
    kernel = jnp.exp(-cost / entropic).reshape(KERNELS, STATES, STATES)
    target = marginals.reshape(KERNELS, STATES)
    scaling = jnp.ones((KERNELS, STATES), jnp.float32)
    last_scaling = jnp.ones((STATES,), jnp.float32)
    for sweep_index in range(SWEEPS):
        alphas = [jnp.ones((STATES,), jnp.float32)]
        for position in range(KERNELS):
            message = jnp.dot(scaling[position] * alphas[position], kernel[position],
                              precision=lax.Precision.HIGHEST, preferred_element_type=jnp.float32)
            alphas.append(message * (STATES / jnp.sum(message)))
        betas = [jnp.ones((STATES,), jnp.float32) for position in range(KERNELS)]
        carried = last_scaling
        for position in reversed(range(KERNELS)):
            message = jnp.dot(kernel[position], carried,
                              precision=lax.Precision.HIGHEST, preferred_element_type=jnp.float32)
            betas[position] = message * (STATES / jnp.sum(message))
            carried = scaling[position] * betas[position]
        scaling = target / (jnp.stack(alphas[:KERNELS]) * jnp.stack(betas))
        last_scaling = final_marginal / alphas[KERNELS]
    return jnp.log(scaling).reshape(KERNELS * STATES)
```

```python
import functools
import math

import jax
import jax.numpy as jnp
from jax import lax
from jax.experimental import pallas as pl
from jax.experimental.pallas import tpu as pltpu
from jax.sharding import PartitionSpec as P

ENTROPIC = 0.25
LANES = 128
SUBLANES = 8
CHUNKS = 8
OWNERS = 2
MESH = pl.DeviceIdType.MESH


def eye():
    shape = (LANES, LANES)
    return lax.broadcasted_iota(jnp.int32, shape, 0) == lax.broadcasted_iota(jnp.int32, shape, 1)


def total(x):
    return jnp.sum(jnp.sum(x, axis=0, keepdims=True), axis=1, keepdims=True)


def chain_kernel(
    width, kernels, cost, marginals, final, out,
    kernel, column, row_sums, marg, fin, alpha, beta, scaling, w0,
    rs_out, rs_in, ag_out, col_in, f0_out, f0_in, f1_out, f1_in, b0_out, b0_in, w1_out, w1_in, ar_in, ls_out, ls_sent,
    load_sem, send_sem, recv_sem,
):
    rows, states = kernel.shape
    blocks = states // LANES
    piece = rows // LANES
    half = width // OWNERS
    me = lax.axis_index("chain")
    g = me // width
    m = me % width
    start = g * width
    last = g == kernels - 1

    def copy(src, dst, slot, target):
        return pltpu.make_async_remote_copy(
            src_ref=src, dst_ref=dst, send_sem=send_sem.at[slot], recv_sem=recv_sem.at[slot],
            device_id={"chain": target}, device_id_type=MESH,
        )

    def received(ref, slot):
        copy(ref, ref, slot, me).wait_recv()

    def sent(ref, slot):
        copy(ref, ref, slot, me).wait_send()

    barrier = pltpu.get_barrier_semaphore()

    def greet(target):
        pl.semaphore_signal(barrier, inc=1, device_id={"chain": target}, device_id_type=MESH)

    @pl.loop(0, width)
    def _(i):
        @pl.when(i != m)
        def _():
            greet(start + i)

        @pl.when(g > 0)
        def _():
            greet(start - width + i)

        @pl.when(g < kernels - 1)
        def _():
            greet(start + width + i)

    span = rows // CHUNKS

    def load(c):
        part = pl.ds(c * span, span)
        return pltpu.make_async_copy(cost.at[part], kernel.at[part], load_sem.at[c])

    for c in range(CHUNKS):
        load(c).start()
    marg_load = pltpu.make_async_copy(marginals, marg, load_sem.at[CHUNKS])
    fin_load = pltpu.make_async_copy(final, fin, load_sem.at[CHUNKS + 1])
    marg_load.start()
    fin_load.start()

    lane = [slice(b * LANES, (b + 1) * LANES) for b in range(blocks)]

    def row_of_column(ref):
        parts = []
        for h in range(piece):
            x = ref[h * LANES : (h + 1) * LANES, :]
            parts.append(jnp.sum(jnp.where(eye(), x, 0.0), axis=0, keepdims=True))
        return jnp.concatenate(parts, axis=0)

    def column_of_row(value):
        for h in range(piece):
            x = jnp.broadcast_to(value[h : h + 1, :], (LANES, LANES))
            x = jnp.sum(jnp.where(eye(), x, 0.0), axis=1, keepdims=True)
            column[h * LANES : (h + 1) * LANES, :] = jnp.broadcast_to(x, (LANES, LANES))

    def tree(values):
        while len(values) > 1:
            values = [a + b for a, b in zip(values[::2], values[1::2])] + values[len(values) // 2 * 2 :]
        return values[0]

    def put_pieces(acc, ref):
        whole = []
        for i in range(width):
            rows_of = [jnp.sum(acc[i * piece + h], axis=0, keepdims=True) for h in range(piece)]
            whole += rows_of
            for h in range(piece):
                ref[i, h : h + 1, :] = rows_of[h]
        whole = tree(whole)
        for i in range(width):
            ref[i, piece : piece + 1, :] = whole

    def sum_pieces(ref):
        x = tree([ref[i] for i in range(width)])
        return x[:piece], total(x[piece:])

    def forward(ref):
        def step(r, acc):
            at = pl.ds(pl.multiple_of(r * SUBLANES, SUBLANES), SUBLANES)
            v = column[at, :]
            return tuple(a + kernel[at, l] * v for a, l in zip(acc, lane))

        zero = tuple(jnp.zeros((SUBLANES, LANES), jnp.float32) for _ in lane)
        put_pieces(lax.fori_loop(0, rows // SUBLANES, step, zero, unroll=2), ref)

    def backward(w):
        ws = [jnp.broadcast_to(w(b), (SUBLANES, LANES)) for b in range(blocks)]

        def step(r, carry):
            at = pl.ds(pl.multiple_of(r * SUBLANES, SUBLANES), SUBLANES)
            x = tree([tree([kernel[at, lane[b]] * ws[b] for b in range(q, q + 8)]) for q in range(0, blocks, 8)])
            column[at, :] = jnp.broadcast_to(jnp.sum(x, axis=1, keepdims=True), (SUBLANES, LANES))
            return carry

        lax.fori_loop(0, rows // SUBLANES, step, 0, unroll=2)
        return row_of_column(column)

    rate = -math.log2(math.e) / ENTROPIC

    def chunk_step(r, acc):
        at = pl.ds(pl.multiple_of(r * SUBLANES, SUBLANES), SUBLANES)
        new = []
        xs = []
        for a, l in zip(acc, lane):
            x = jnp.exp2(kernel[at, l] * rate)
            kernel[at, l] = x
            xs.append(x)
            new.append(a + x)
        x = tree(xs)
        row_sums[at, :] = jnp.broadcast_to(jnp.sum(x, axis=1, keepdims=True), (SUBLANES, LANES))
        return tuple(new)

    acc = tuple(jnp.zeros((SUBLANES, LANES), jnp.float32) for _ in lane)
    for c in range(CHUNKS):
        load(c).wait()
        acc = lax.fori_loop(c * span // SUBLANES, (c + 1) * span // SUBLANES, chunk_step, acc)
    put_pieces(acc, rs_out)

    greeted = width - 1 + width * ((g > 0).astype(jnp.int32) + (g < kernels - 1).astype(jnp.int32))
    pl.semaphore_wait(barrier, greeted)

    RS, AG, F0, F1, B0, W1, AR, LS = range(8)

    def to_group(src, dst, slot, group, first):
        @pl.loop(0, width)
        def _(j):
            i = width - 1 - j if first == "high" else j
            copy(src(i), dst.at[m], slot, group * width + i).start()

    def to_own(src, dst, slot):
        @pl.loop(1, width)
        def _(j):
            i = (m + j) % width
            copy(src(i), dst.at[m], slot, start + i).start()

    @pl.when(g == 0)
    def _():
        to_group(lambda i: rs_out.at[i], f0_in, F0, g + 1, "high")

    @pl.when(last)
    def _():
        b = row_of_column(row_sums)
        beta[...] = b
        b0_out[0:piece, :] = b
        b0_out[piece : piece + 1, :] = jnp.sum(b, axis=0, keepdims=True)
        to_group(lambda i: b0_out, b0_in, B0, g - 1, "low")

    to_own(lambda i: rs_out.at[i], rs_in, RS)
    rs_in[m] = rs_out[m]
    received(rs_in.at[pl.ds(0, width - 1)], RS)
    block, _ = sum_pieces(rs_in)
    ag_out[...] = block
    col_in[m] = block
    to_own(lambda i: ag_out, col_in, AG)

    marg_load.wait()
    fin_load.wait()
    scaling[...] = jnp.ones_like(scaling)
    alpha[...] = jnp.ones_like(alpha)

    def forward_0():
        received(f0_in, F0)
        a, s = sum_pieces(f0_in)
        a = a * (states / s)
        alpha[...] = a
        column_of_row(a)
        forward(f0_out)

    def set_beta(b, w):
        s = total(jnp.sum(col_in[...] * w, axis=0))
        beta[...] = b * (states / s)

    @pl.when(g == 1)
    def _():
        forward_0()
        to_group(lambda i: f0_out.at[i], f0_in, F0, g + 1, "high")

    received(col_in.at[pl.ds(0, width - 1)], AG)

    @pl.when(jnp.logical_not(last))
    def _():
        received(b0_in, B0)
        x = b0_in[...]
        s = total(tree([x[i, piece:] for i in range(width)]))
        w = x[:, :piece] * (states / s)
        w0[...] = w
        b = backward(lambda k: w0[k // piece, k % piece : k % piece + 1, :])

        @pl.when(g > 0)
        def _():
            b0_out[0:piece, :] = b
            b0_out[piece : piece + 1, :] = jnp.sum(b, axis=0, keepdims=True)
            to_group(lambda i: b0_out, b0_in, B0, g - 1, "low")

        set_beta(b, w)

    @pl.when(last)
    def _():
        set_beta(beta[...], jnp.ones((width, piece, LANES), jnp.float32))

    @pl.when(g > 1)
    def _():
        forward_0()

    @pl.when(jnp.logical_and(g > 1, jnp.logical_not(last)))
    def _():
        to_group(lambda i: f0_out.at[i], f0_in, F0, g + 1, "high")

    @pl.when(last)
    def _():
        for o in range(OWNERS):
            part = pl.ds(o * half, half)
            owner = width - OWNERS + o

            @pl.when(m != owner)
            def _():
                copy(f0_out.at[part], ar_in.at[m], AR, start + owner).start()

        for o in range(OWNERS):
            part = pl.ds(o * half, half)
            owner = width - OWNERS + o

            @pl.when(m == owner)
            def _():
                ar_in[m] = f0_out[part]
                received(ar_in.at[pl.ds(0, width - 1)], AR)
                x = tree([ar_in[i] for i in range(width)])
                s = total(x[0, piece:])
                ls = fin[part] / (x[:, :piece] * (states / s))
                ls_out[...] = ls
                w1_in[part] = ls

                @pl.loop(0, width)
                def _(i):
                    @pl.when(i != owner)
                    def _():
                        copy(ls_out, w1_in.at[part], LS, start + i).start()

                for other in range(OWNERS):
                    if other != o:
                        received(w1_in.at[pl.ds(other * half, half)], LS)

        @pl.when(m < width - OWNERS)
        def _():
            received(w1_in, LS)

    scaling[...] = marg[...] / (alpha[...] * beta[...])

    def backward_1():
        w = w1_in[...]
        b = backward(lambda k: w1_in[k // piece, k % piece : k % piece + 1, :])
        set_beta(b, w)

        @pl.when(g > 0)
        def _():
            w1_out[...] = scaling[...] * beta[...]
            to_group(lambda i: w1_out, w1_in, W1, g - 1, "low")

    @pl.when(last)
    def _():
        backward_1()

    @pl.when(g > 0)
    def _():
        received(f1_in, F1)
        a, s = sum_pieces(f1_in)
        alpha[...] = a * (states / s)

    @pl.when(jnp.logical_not(last))
    def _():
        column_of_row(scaling[...] * alpha[...])
        forward(f1_out)
        to_group(lambda i: f1_out.at[i], f1_in, F1, g + 1, "high")
        received(w1_in, W1)
        backward_1()

    out[...] = marg[...] / (alpha[...] * beta[...])

    sent(rs_in.at[pl.ds(0, width - 1)], RS)
    sent(col_in.at[pl.ds(0, width - 1)], AG)

    @pl.when(jnp.logical_not(last))
    def _():
        sent(f0_in, F0)
        sent(f1_in, F1)

    @pl.when(g > 0)
    def _():
        sent(b0_in, B0)
        sent(w1_in, W1)

    @pl.when(last)
    def _():
        for o in range(OWNERS):
            owner = width - OWNERS + o

            @pl.when(m != owner)
            def _():
                sent(ar_in.at[m], AR)

            @pl.when(m == owner)
            def _():
                sent(ls_sent, LS)


def solution(mesh):
    chain = mesh.shape["chain"]

    def on_device(cost, marginals, final_marginal):
        rows, states = cost.shape
        width = states // rows
        piece = rows // LANES

        def buffer(*shape):
            return pltpu.VMEM(shape + (LANES,), jnp.float32)

        pieces = buffer(width, piece + 1)
        whole = buffer(width, piece)
        one = buffer(piece)
        half = width // OWNERS
        scratch = [
            pltpu.VMEM((rows, states), jnp.float32), buffer(rows), buffer(rows),
            one, whole, one, one, one, whole,
            pieces, pieces, one, whole, pieces, pieces, pieces, pieces, buffer(piece + 1), pieces, one, whole,
            buffer(width, half, piece + 1), buffer(half, piece), buffer(width - 1, half, piece),
            pltpu.SemaphoreType.DMA((CHUNKS + 2,)), pltpu.SemaphoreType.DMA((8,)), pltpu.SemaphoreType.DMA((8,)),
        ]
        scaling = pl.pallas_call(
            functools.partial(chain_kernel, width, chain // width),
            out_shape=jax.ShapeDtypeStruct((piece, LANES), jnp.float32),
            in_specs=[pl.BlockSpec(memory_space=pl.ANY)] * 3,
            out_specs=pl.BlockSpec(memory_space=pltpu.VMEM),
            scratch_shapes=scratch,
            compiler_params=pltpu.CompilerParams(collective_id=0, has_side_effects=True),
            name="sinkhorn_chain",
        )(cost, marginals.reshape(piece, LANES), final_marginal.reshape(width, piece, LANES))
        return jnp.log(scaling).reshape(rows)

    placed = (P(("pop", "chain"), None), P(("pop", "chain")), P("pop"))
    return jax.shard_map(on_device, mesh=mesh, in_specs=placed, out_specs=P(("pop", "chain")), check_vma=False)
```

```python
import functools
import math

import jax
import jax.numpy as jnp
from jax import lax
from jax.experimental import pallas as pl
from jax.experimental.pallas import tpu as pltpu
from jax.sharding import PartitionSpec as P

ENTROPIC = 0.25
LANES = 128
SUBLANES = 8
CHUNKS = 8
CORES = 2
QUARTERS = 4
MESH = pl.DeviceIdType.MESH
SLOTS = range(17)
KX, PK, RX, MX, CS, CB, A1, F0, AR, LS, B0, W1, F1, AX, BX, AO, BO = SLOTS


def eye():
    shape = (LANES, LANES)
    return lax.broadcasted_iota(jnp.int32, shape, 0) == lax.broadcasted_iota(jnp.int32, shape, 1)


def total(x):
    return jnp.sum(jnp.sum(x, axis=0, keepdims=True), axis=1, keepdims=True)


def tree(values):
    while len(values) > 1:
        values = [a + b for a, b in zip(values[::2], values[1::2])] + values[len(values) // 2 * 2 :]
    return values[0]


def signal(sem, target):
    pl.semaphore_signal(sem, inc=1, device_id={"chain": target}, device_id_type=MESH)


def chain_kernel(
    width, kernels, cost, marginals, final, out,
    kernel, column, marg, fin, row_out, row_in, rsum, col_out, col_mate, col_in, cs_in, many,
    a1_in, f_out, f0_in, f1_in, ar_in, b0_out, b0_in, w0, w1_out, w1_in,
    alpha, alpha_in, beta, beta_in, alpha_last, beta_last,
    load_sem, send_sem, recv_sem, token,
):
    states = kernel.shape[1]
    rows = kernel.shape[0] // CORES
    blocks = states // LANES
    piece = kernel.shape[0] // LANES
    chips = width // CORES
    me = lax.axis_index("chain")
    g = me // width
    m = me % width
    chip = m // CORES
    core = m % CORES
    mate = me + 1 - 2 * core
    start = g * width
    first_g, last_g = g == 0, g == kernels - 1
    lead = core == 1
    up_collector = jnp.logical_and(lead, chip == chips - 1)
    down_collector = jnp.logical_and(lead, chip == 0)
    owner = start + width - 1

    def when(condition):
        return pl.when(condition)

    def both(*conditions):
        return functools.reduce(jnp.logical_and, conditions)

    def no(condition):
        return jnp.logical_not(condition)

    def copy(src, dst, slot, target):
        return pltpu.make_async_remote_copy(
            src_ref=src, dst_ref=dst, send_sem=send_sem.at[slot], recv_sem=recv_sem.at[slot],
            device_id={"chain": target}, device_id_type=MESH,
        )

    def received(ref, slot):
        copy(ref, ref, slot, mate).wait_recv()

    def sent(ref, slot):
        copy(ref, ref, slot, mate).wait_send()

    barrier = pltpu.get_barrier_semaphore()
    signal(barrier, mate)

    @when(both(me != owner, mate != owner))
    def _():
        signal(barrier, owner)

    @when(both(me != start + 1, mate != start + 1))
    def _():
        signal(barrier, start + 1)

    @when(no(first_g))
    def _():
        signal(barrier, owner - width)

    @when(no(last_g))
    def _():
        signal(barrier, start + width + 1)

    @when(up_collector)
    def _():
        for i in range(1, chips - 1):
            signal(barrier, start + CORES * i + 1)

    span = rows // CHUNKS
    base = core * rows

    def load(c):
        return pltpu.make_async_copy(
            cost.at[pl.ds(c * span, span)], kernel.at[pl.ds(base + c * span, span)], load_sem.at[c]
        )

    for c in range(CHUNKS):
        load(c).start()
    marg_load = pltpu.make_async_copy(marginals, marg.at[core], load_sem.at[CHUNKS])
    fin_load = pltpu.make_async_copy(final, fin, load_sem.at[CHUNKS + 1])
    marg_load.start()
    fin_load.start()

    def lanes(b):
        return slice(b * LANES, (b + 1) * LANES)

    def row_of_column(ref, count):
        parts = []
        for h in range(count):
            x = ref[h * LANES : (h + 1) * LANES, :]
            parts.append(jnp.sum(jnp.where(eye(), x, 0.0), axis=0, keepdims=True))
        return jnp.concatenate(parts, axis=0)

    def column_of_row(value):
        for h in range(piece):
            x = jnp.broadcast_to(value[h : h + 1, :], (LANES, LANES))
            x = jnp.sum(jnp.where(eye(), x, 0.0), axis=1, keepdims=True)
            column[h * LANES : (h + 1) * LANES, :] = jnp.broadcast_to(x, (LANES, LANES))

    def forward(v, order, send):
        column_of_row(v)
        row = jnp.sum(v * rsum[...], axis=0, keepdims=True)
        quarters = min(QUARTERS, chips)
        for q in range(quarters):
            targets = order[q * chips // quarters : (q + 1) * chips // quarters]
            mine = [i * piece + h for i in targets for h in range(piece)]

            def step(r, acc):
                at = pl.ds(pl.multiple_of(r * SUBLANES, SUBLANES), SUBLANES)
                v = column[at, :]
                return tuple(a + kernel[at, lanes(b)] * v for a, b in zip(acc, mine))

            zero = tuple(jnp.zeros((SUBLANES, LANES), jnp.float32) for _ in mine)
            acc = lax.fori_loop(0, CORES * rows // SUBLANES, step, zero, unroll=8)
            for n, i in enumerate(targets):
                for h in range(piece):
                    f_out[i, h : h + 1, :] = jnp.sum(acc[n * piece + h], axis=0, keepdims=True)
                f_out[i, piece : piece + 1, :] = row
            for i in targets:
                send(i)

    def backward(ref):
        ws = [
            jnp.broadcast_to(ref[b // piece, b % piece : b % piece + 1, :], (SUBLANES, LANES)) for b in range(blocks)
        ]

        def step(r, carry):
            at = pl.ds(pl.multiple_of(r * SUBLANES, SUBLANES), SUBLANES)
            x = tree([tree([kernel[at, lanes(b)] * ws[b] for b in range(q, q + 8)]) for q in range(0, blocks, 8)])
            column[at, :] = jnp.broadcast_to(jnp.sum(x, axis=1, keepdims=True), (SUBLANES, LANES))
            return carry

        lax.fori_loop(0, CORES * rows // SUBLANES, step, 0, unroll=4)
        return row_of_column(column, piece)

    def sum_pieces(ref):
        x = tree([ref[i] for i in range(chips)])
        return x[:piece], total(x[piece:])

    rate = -math.log2(math.e) / ENTROPIC

    def chunk_step(r, acc):
        at = pl.ds(pl.multiple_of(base + r * SUBLANES, SUBLANES), SUBLANES)
        new, xs = [], []
        for b in range(blocks):
            x = jnp.exp2(kernel[at, lanes(b)] * rate)
            kernel[at, lanes(b)] = x
            xs.append(x)
            new.append(acc[b] + x)
        here = pl.ds(pl.multiple_of(r * SUBLANES, SUBLANES), SUBLANES)
        column[here, :] = jnp.broadcast_to(jnp.sum(tree(xs), axis=1, keepdims=True), (SUBLANES, LANES))
        return tuple(new)

    acc = tuple(jnp.zeros((SUBLANES, LANES), jnp.float32) for _ in range(blocks))
    for c in range(CHUNKS):
        load(c).wait()
        acc = lax.fori_loop(c * span // SUBLANES, (c + 1) * span // SUBLANES, chunk_step, acc)
    for b in range(blocks):
        col_out[b // piece, b % piece : b % piece + 1, :] = jnp.sum(acc[b], axis=0, keepdims=True)
    row_out[...] = row_of_column(column, piece // CORES)
    marg_load.wait()
    fin_load.wait()

    greeted = jnp.where(lead, 2, 1)
    greeted = jnp.where(down_collector, width - 1 + jnp.where(first_g, 0, width), greeted)
    greeted = jnp.where(up_collector, width - 1 + jnp.where(last_g, 0, width), greeted)
    pl.semaphore_wait(barrier, greeted)

    @when(no(lead))
    def _():
        copy(col_out, col_mate, PK, mate).start()

    copy(row_out, row_in, RX, mate).start()
    copy(marg.at[core], marg.at[core], MX, mate).start()
    half = kernel.at[pl.ds(base, rows)]
    copy(half, half, KX, mate).start()

    UP, DOWN = 0, 1

    @when(both(up_collector, no(last_g)))
    def _():
        for i in range(width - 1):
            signal(token.at[UP], start + i)

    @when(both(down_collector, no(first_g)))
    def _():
        for i in range(width):
            if i != 1:
                signal(token.at[DOWN], start + i)

    def wait_up():
        @when(both(no(up_collector), no(last_g)))
        def _():
            pl.semaphore_wait(token.at[UP], 1)

    def wait_down():
        @when(both(no(down_collector), no(first_g)))
        def _():
            pl.semaphore_wait(token.at[DOWN], 1)

    def to_group(src, dst, slot, group, i):
        copy(src, dst.at[chip], slot, group * width + CORES * i + core).start()

    high = list(range(chips - 1, -1, -1))
    low = list(range(chips))

    @when(lead)
    def _():
        received(col_mate, PK)
        col_out[...] = col_out[...] + col_mate[...]

    @when(both(lead, no(up_collector)))
    def _():
        copy(col_out, cs_in.at[chip], CS, owner).start()

    @when(up_collector)
    def _():
        cs_in[chips - 1] = col_out[...]
        received(cs_in.at[pl.ds(0, chips - 1)], CS)
        c = tree([cs_in[i] for i in range(chips)])
        col_in[...] = c

        @when(first_g)
        def _():
            w1_out[...] = c * (states / total(jnp.sum(c, axis=0)))
            for i in high:
                copy(w1_out.at[i], a1_in, A1, start + width + CORES * i + 1).start()

        for i in range(width - 1):
            copy(col_in, col_in, CB, start + i).start()

    received(row_in, RX)

    @when(lead)
    def _():
        rsum[...] = jnp.concatenate([row_in[...], row_out[...]], axis=0)

    @when(no(lead))
    def _():
        rsum[...] = jnp.concatenate([row_out[...], row_in[...]], axis=0)

    received(marg.at[1 - core], MX)
    target = jnp.concatenate([marg[i] for i in range(CORES)], axis=0)

    def set_beta(ref, b, w):
        s = total(jnp.sum(col_in[...] * w, axis=0))
        ref[...] = b * (states / s)

    @when(lead)
    def _():
        alpha[...] = jnp.ones_like(alpha)

        @when(g == 1)
        def _():
            received(a1_in, A1)
            alpha[...] = a1_in[...]

        @when(g > 1)
        def _():
            received(f0_in, F0)
            a, s = sum_pieces(f0_in)
            alpha[...] = a * (states / s)

        received(kernel.at[pl.ds(0, rows)], KX)
        wait_up()

        @when(no(first_g))
        def _():
            def send(i):
                @when(no(last_g))
                def _():
                    to_group(f_out.at[i], f0_in, F0, g + 1, i)

            forward(alpha[...], high, send)
            copy(alpha, alpha_in, AX, mate).start()

        @when(both(last_g, no(up_collector)))
        def _():
            copy(f_out, ar_in.at[chip], AR, owner).start()
            received(w1_in, LS)

        @when(both(last_g, up_collector))
        def _():
            ar_in[chips - 1] = f_out[...]
            received(ar_in.at[pl.ds(0, chips - 1)], AR)
            x = tree([ar_in[i] for i in range(chips)])[:, :piece]
            w1_in[...] = fin[...] / (x * (states / total(jnp.sum(x, axis=0))))
            for i in range(chips - 1):
                copy(w1_in, w1_in, LS, start + CORES * i + 1).start()

        @when(no(up_collector))
        def _():
            received(col_in, CB)

        received(beta_in, BX)
        scaling = target / (alpha[...] * beta_in[...])

        @when(no(last_g))
        def _():
            received(w1_in, W1)

        b = backward(w1_in)
        set_beta(beta_last, b, w1_in[...])
        wait_down()

        @when(no(first_g))
        def _():
            w1_out[0] = scaling * beta_last[...]
            for i in low:
                to_group(w1_out.at[0], w1_in, W1, g - 1, i)

        copy(beta_last, beta_last, BO, mate).start()
        received(alpha_last, AO)

    @when(no(lead))
    def _():
        def send_b(b):
            b0_out[0:piece, :] = b
            b0_out[piece : piece + 1, :] = jnp.sum(b, axis=0, keepdims=True)
            wait_down()
            for i in low:
                to_group(b0_out, b0_in, B0, g - 1, i)

        @when(last_g)
        def _():
            send_b(rsum[...])
            received(col_in, CB)
            set_beta(beta, rsum[...], jnp.ones((chips, piece, LANES), jnp.float32))

        received(kernel.at[pl.ds(rows, rows)], KX)

        @when(no(last_g))
        def _():
            received(b0_in, B0)
            x = b0_in[...]
            s = total(tree([x[i, piece:] for i in range(chips)]))
            w0[...] = x[:, :piece] * (states / s)
            b = backward(w0)

            @when(no(first_g))
            def _():
                send_b(b)

            received(col_in, CB)
            set_beta(beta, b, w0[...])

        copy(beta, beta_in, BX, mate).start()
        alpha_last[...] = jnp.ones_like(alpha_last)
        alpha_in_value = jnp.ones((piece, LANES), jnp.float32)

        @when(first_g)
        def _():
            alpha_in[...] = alpha_in_value

        @when(no(first_g))
        def _():
            received(alpha_in, AX)
            received(f1_in, F1)
            a, s = sum_pieces(f1_in)
            alpha_last[...] = a * (states / s)

        copy(alpha_last, alpha_last, AO, mate).start()
        wait_up()

        @when(no(last_g))
        def _():
            scaling = target / (alpha_in[...] * beta[...])
            forward(scaling * alpha_last[...], high, lambda i: to_group(f_out.at[i], f1_in, F1, g + 1, i))

        received(beta_last, BO)

    result = target / (alpha_last[...] * beta_last[...])
    out[...] = jnp.where(lead, result[piece // CORES :], result[: piece // CORES])

    sent(row_in, RX)
    sent(marg.at[core], MX)
    sent(half, KX)

    @when(lead)
    def _():
        sent(beta_last, BO)

        @when(no(up_collector))
        def _():
            sent(col_out, CS)

        @when(up_collector)
        def _():
            sent(many, CB)

            @when(first_g)
            def _():
                sent(col_in, A1)

        @when(both(g > 0, no(last_g)))
        def _():
            sent(f0_in, F0)

        @when(no(first_g))
        def _():
            sent(alpha, AX)
            sent(w1_in, W1)

        @when(both(last_g, no(up_collector)))
        def _():
            sent(f_out, AR)

        @when(both(last_g, up_collector))
        def _():
            sent(many.at[pl.ds(0, chips - 1)], LS)

    @when(no(lead))
    def _():
        sent(col_out, PK)
        sent(beta, BX)
        sent(alpha_last, AO)

        @when(no(first_g))
        def _():
            sent(b0_in, B0)

        @when(no(last_g))
        def _():
            sent(f1_in, F1)


def solution(mesh):
    chain = mesh.shape["chain"]

    def on_device(cost, marginals, final_marginal):
        rows, states = cost.shape
        width = states // rows
        chips = width // CORES
        own = rows // LANES
        piece = CORES * own

        def buffer(*shape):
            return pltpu.VMEM(shape + (LANES,), jnp.float32)

        one = buffer(piece)
        whole = buffer(chips, piece)
        pieces = buffer(chips, piece + 1)
        scratch = dict(
            kernel=pltpu.VMEM((CORES * rows, states), jnp.float32), column=buffer(CORES * rows),
            marg=buffer(CORES, own), fin=whole, row_out=buffer(own), row_in=buffer(own), rsum=one,
            col_out=whole, col_mate=whole, col_in=whole, cs_in=buffer(chips, chips, piece),
            many=buffer(width - 1, chips, piece),
            a1_in=one, f_out=pieces, f0_in=pieces, f1_in=pieces, ar_in=buffer(chips, chips, piece + 1),
            b0_out=buffer(piece + 1), b0_in=pieces, w0=whole, w1_out=whole, w1_in=whole,
            alpha=one, alpha_in=one, beta=one, beta_in=one, alpha_last=one, beta_last=one,
            load_sem=pltpu.SemaphoreType.DMA((CHUNKS + 2,)), send_sem=pltpu.SemaphoreType.DMA((len(SLOTS),)),
            recv_sem=pltpu.SemaphoreType.DMA((len(SLOTS),)), token=pltpu.SemaphoreType.REGULAR((2,)),
        )
        scaling = pl.pallas_call(
            functools.partial(chain_kernel, width, chain // width),
            out_shape=jax.ShapeDtypeStruct((own, LANES), jnp.float32),
            in_specs=[pl.BlockSpec(memory_space=pl.ANY)] * 3,
            out_specs=pl.BlockSpec(memory_space=pltpu.VMEM),
            scratch_shapes=scratch,
            compiler_params=pltpu.CompilerParams(collective_id=0, has_side_effects=True),
            name="sinkhorn_chain",
        )(cost, marginals.reshape(own, LANES), final_marginal.reshape(chips, piece, LANES))
        return jnp.log(scaling).reshape(rows)

    placed = (P(("pop", "chain"), None), P(("pop", "chain")), P("pop"))
    return jax.shard_map(on_device, mesh=mesh, in_specs=placed, out_specs=P(("pop", "chain")), check_vma=False)
```

```python
import functools
import math

import jax
import jax.numpy as jnp
from jax import lax
from jax.experimental import pallas as pl
from jax.experimental.pallas import tpu as pltpu
from jax.sharding import PartitionSpec as P

ENTROPIC = 0.25
LANES = 128
SUBLANES = 8
CHUNKS = 8
CORES = 2
QUARTERS = 4
MESH = pl.DeviceIdType.MESH
SLOTS = range(17)
KX, PK, RX, MX, CS, CB, A1, F0, AR, LS, B0, W1, F1, AX, BX, AO, BO = SLOTS


def eye():
    shape = (LANES, LANES)
    return lax.broadcasted_iota(jnp.int32, shape, 0) == lax.broadcasted_iota(jnp.int32, shape, 1)


def total(x):
    return jnp.sum(jnp.sum(x, axis=0, keepdims=True), axis=1, keepdims=True)


def tree(values):
    while len(values) > 1:
        values = [a + b for a, b in zip(values[::2], values[1::2])] + values[len(values) // 2 * 2 :]
    return values[0]


def signal(sem, target):
    pl.semaphore_signal(sem, inc=1, device_id={"chain": target}, device_id_type=MESH)


def chain_kernel(
    width, kernels, cost, marginals, final, out,
    kernel, column, marg, fin, row_out, row_in, rsum, col_out, col_mate, col_in, cs_in, many,
    a1_in, f_out, f0_in, f1_in, ar_in, b0_out, b0_in, w0, w1_out, w1_in,
    alpha, alpha_in, beta, beta_in, alpha_last, beta_last,
    load_sem, send_sem, recv_sem, token,
):
    states = kernel.shape[1]
    rows = kernel.shape[0] // CORES
    blocks = states // LANES
    piece = kernel.shape[0] // LANES
    chips = width // CORES
    me = lax.axis_index("chain")
    g = me // width
    m = me % width
    chip = m // CORES
    core = m % CORES
    mate = me + 1 - 2 * core
    start = g * width
    first_g, last_g = g == 0, g == kernels - 1
    lead = core == 1
    up_collector = jnp.logical_and(lead, chip == chips - 1)
    down_collector = jnp.logical_and(lead, chip == 0)
    owner = start + width - 1

    def when(condition):
        return pl.when(condition)

    def both(*conditions):
        return functools.reduce(jnp.logical_and, conditions)

    def no(condition):
        return jnp.logical_not(condition)

    def copy(src, dst, slot, target):
        return pltpu.make_async_remote_copy(
            src_ref=src, dst_ref=dst, send_sem=send_sem.at[slot], recv_sem=recv_sem.at[slot],
            device_id={"chain": target}, device_id_type=MESH,
        )

    def received(ref, slot):
        copy(ref, ref, slot, mate).wait_recv()

    def sent(ref, slot):
        copy(ref, ref, slot, mate).wait_send()

    barrier = pltpu.get_barrier_semaphore()
    signal(barrier, mate)

    @when(both(me != owner, mate != owner))
    def _():
        signal(barrier, owner)

    @when(both(me != start + 1, mate != start + 1))
    def _():
        signal(barrier, start + 1)

    @when(no(first_g))
    def _():
        signal(barrier, owner - width)

    @when(no(last_g))
    def _():
        signal(barrier, start + width + 1)

    @when(up_collector)
    def _():
        for i in range(1, chips - 1):
            signal(barrier, start + CORES * i + 1)

    span = rows // CHUNKS
    base = core * rows

    def load(c):
        return pltpu.make_async_copy(
            cost.at[pl.ds(c * span, span)], kernel.at[pl.ds(base + c * span, span)], load_sem.at[c]
        )

    for c in range(CHUNKS):
        load(c).start()
    marg_load = pltpu.make_async_copy(marginals, marg.at[core], load_sem.at[CHUNKS])
    fin_load = pltpu.make_async_copy(final, fin, load_sem.at[CHUNKS + 1])
    marg_load.start()
    fin_load.start()

    def lanes(b):
        return slice(b * LANES, (b + 1) * LANES)

    def row_of_column(ref, count):
        parts = []
        for h in range(count):
            x = jnp.sum(ref[h * LANES : (h + 1) * LANES, :], axis=1, keepdims=True)
            parts.append(jnp.sum(jnp.where(eye(), x, 0.0), axis=0, keepdims=True))
        return jnp.concatenate(parts, axis=0)

    def column_of_row(value):
        for h in range(piece):
            x = jnp.broadcast_to(value[h : h + 1, :], (LANES, LANES))
            x = jnp.sum(jnp.where(eye(), x, 0.0), axis=1, keepdims=True)
            column[h * LANES : (h + 1) * LANES, :] = jnp.broadcast_to(x, (LANES, LANES))

    def forward(v, order, send):
        column_of_row(v)
        row = jnp.sum(v * rsum[...], axis=0, keepdims=True)
        quarters = min(QUARTERS, chips)
        for q in range(quarters):
            targets = order[q * chips // quarters : (q + 1) * chips // quarters]
            mine = [i * piece + h for i in targets for h in range(piece)]

            def step(r, acc):
                at = pl.ds(pl.multiple_of(r * SUBLANES, SUBLANES), SUBLANES)
                v = column[at, :]
                return tuple(a + kernel[at, lanes(b)] * v for a, b in zip(acc, mine))

            zero = tuple(jnp.zeros((SUBLANES, LANES), jnp.float32) for _ in mine)
            acc = lax.fori_loop(0, CORES * rows // SUBLANES, step, zero, unroll=8)
            for n, i in enumerate(targets):
                for h in range(piece):
                    f_out[i, h : h + 1, :] = jnp.sum(acc[n * piece + h], axis=0, keepdims=True)
                f_out[i, piece : piece + 1, :] = row
            for i in targets:
                send(i)

    def backward(ref):
        ws = [
            jnp.broadcast_to(ref[b // piece, b % piece : b % piece + 1, :], (SUBLANES, LANES)) for b in range(blocks)
        ]

        def step(r, carry):
            at = pl.ds(pl.multiple_of(r * SUBLANES, SUBLANES), SUBLANES)
            x = [kernel[at, lanes(b)] * ws[b] for b in range(4)]
            for b in range(4, blocks):
                x[b % 4] = x[b % 4] + kernel[at, lanes(b)] * ws[b]
            column[at, :] = tree(x)
            return carry

        lax.fori_loop(0, CORES * rows // SUBLANES, step, 0, unroll=8)
        return row_of_column(column, piece)

    def sum_pieces(ref):
        x = tree([ref[i] for i in range(chips)])
        return x[:piece], total(x[piece:])

    rate = -math.log2(math.e) / ENTROPIC

    def chunk_step(r, acc):
        at = pl.ds(pl.multiple_of(base + r * SUBLANES, SUBLANES), SUBLANES)
        new, xs = [], []
        for b in range(blocks):
            x = jnp.exp2(kernel[at, lanes(b)] * rate)
            kernel[at, lanes(b)] = x
            xs.append(x)
            new.append(acc[b] + x)
        here = pl.ds(pl.multiple_of(r * SUBLANES, SUBLANES), SUBLANES)
        column[here, :] = tree(xs)
        return tuple(new)

    acc = tuple(jnp.zeros((SUBLANES, LANES), jnp.float32) for _ in range(blocks))
    for c in range(CHUNKS):
        load(c).wait()
        acc = lax.fori_loop(c * span // SUBLANES, (c + 1) * span // SUBLANES, chunk_step, acc)
    for b in range(blocks):
        col_out[b // piece, b % piece : b % piece + 1, :] = jnp.sum(acc[b], axis=0, keepdims=True)
    row_out[...] = row_of_column(column, piece // CORES)
    marg_load.wait()
    fin_load.wait()

    greeted = jnp.where(lead, 2, 1)
    greeted = jnp.where(down_collector, width - 1 + jnp.where(first_g, 0, width), greeted)
    greeted = jnp.where(up_collector, width - 1 + jnp.where(last_g, 0, width), greeted)
    pl.semaphore_wait(barrier, greeted)

    @when(no(lead))
    def _():
        copy(col_out, col_mate, PK, mate).start()

    copy(row_out, row_in, RX, mate).start()
    copy(marg.at[core], marg.at[core], MX, mate).start()
    half = kernel.at[pl.ds(base, rows)]
    copy(half, half, KX, mate).start()

    UP, DOWN = 0, 1

    @when(both(up_collector, no(last_g)))
    def _():
        for i in range(width - 1):
            signal(token.at[UP], start + i)

    @when(both(down_collector, no(first_g)))
    def _():
        for i in range(width):
            if i != 1:
                signal(token.at[DOWN], start + i)

    def wait_up():
        @when(both(no(up_collector), no(last_g)))
        def _():
            pl.semaphore_wait(token.at[UP], 1)

    def wait_down():
        @when(both(no(down_collector), no(first_g)))
        def _():
            pl.semaphore_wait(token.at[DOWN], 1)

    def to_group(src, dst, slot, group, i):
        copy(src, dst.at[chip], slot, group * width + CORES * i + core).start()

    high = list(range(chips - 1, -1, -1))
    low = list(range(chips))

    @when(lead)
    def _():
        received(col_mate, PK)
        col_out[...] = col_out[...] + col_mate[...]

    @when(both(lead, no(up_collector)))
    def _():
        copy(col_out, cs_in.at[chip], CS, owner).start()

    @when(up_collector)
    def _():
        cs_in[chips - 1] = col_out[...]
        received(cs_in.at[pl.ds(0, chips - 1)], CS)
        c = tree([cs_in[i] for i in range(chips)])
        col_in[...] = c

        @when(first_g)
        def _():
            w1_out[...] = c * (states / total(jnp.sum(c, axis=0)))
            for i in high:
                copy(w1_out.at[i], a1_in, A1, start + width + CORES * i + 1).start()

        for i in range(width - 1):
            copy(col_in, col_in, CB, start + i).start()

    received(row_in, RX)

    @when(lead)
    def _():
        rsum[...] = jnp.concatenate([row_in[...], row_out[...]], axis=0)

    @when(no(lead))
    def _():
        rsum[...] = jnp.concatenate([row_out[...], row_in[...]], axis=0)

    received(marg.at[1 - core], MX)
    target = jnp.concatenate([marg[i] for i in range(CORES)], axis=0)

    def set_beta(ref, b, w):
        s = total(jnp.sum(col_in[...] * w, axis=0))
        ref[...] = b * (states / s)

    @when(lead)
    def _():
        alpha[...] = jnp.ones_like(alpha)

        @when(g == 1)
        def _():
            received(a1_in, A1)
            alpha[...] = a1_in[...]

        @when(g > 1)
        def _():
            received(f0_in, F0)
            a, s = sum_pieces(f0_in)
            alpha[...] = a * (states / s)

        received(kernel.at[pl.ds(0, rows)], KX)
        wait_up()

        @when(no(first_g))
        def _():
            def send(i):
                @when(no(last_g))
                def _():
                    to_group(f_out.at[i], f0_in, F0, g + 1, i)

            forward(alpha[...], high, send)
            copy(alpha, alpha_in, AX, mate).start()

        @when(both(last_g, no(up_collector)))
        def _():
            copy(f_out, ar_in.at[chip], AR, owner).start()
            received(w1_in, LS)

        @when(both(last_g, up_collector))
        def _():
            ar_in[chips - 1] = f_out[...]
            received(ar_in.at[pl.ds(0, chips - 1)], AR)
            x = tree([ar_in[i] for i in range(chips)])[:, :piece]
            w1_in[...] = fin[...] / (x * (states / total(jnp.sum(x, axis=0))))
            for i in range(chips - 1):
                copy(w1_in, w1_in, LS, start + CORES * i + 1).start()

        @when(no(up_collector))
        def _():
            received(col_in, CB)

        received(beta_in, BX)
        scaling = target / (alpha[...] * beta_in[...])

        @when(no(last_g))
        def _():
            received(w1_in, W1)

        b = backward(w1_in)
        set_beta(beta_last, b, w1_in[...])
        wait_down()

        @when(no(first_g))
        def _():
            w1_out[0] = scaling * beta_last[...]
            for i in low:
                to_group(w1_out.at[0], w1_in, W1, g - 1, i)

        copy(beta_last, beta_last, BO, mate).start()
        received(alpha_last, AO)

    @when(no(lead))
    def _():
        def send_b(b):
            b0_out[0:piece, :] = b
            b0_out[piece : piece + 1, :] = jnp.sum(b, axis=0, keepdims=True)
            wait_down()
            for i in low:
                to_group(b0_out, b0_in, B0, g - 1, i)

        @when(last_g)
        def _():
            send_b(rsum[...])
            received(col_in, CB)
            set_beta(beta, rsum[...], jnp.ones((chips, piece, LANES), jnp.float32))

        received(kernel.at[pl.ds(rows, rows)], KX)

        @when(no(last_g))
        def _():
            received(b0_in, B0)
            x = b0_in[...]
            s = total(tree([x[i, piece:] for i in range(chips)]))
            w0[...] = x[:, :piece] * (states / s)
            b = backward(w0)

            @when(no(first_g))
            def _():
                send_b(b)

            received(col_in, CB)
            set_beta(beta, b, w0[...])

        copy(beta, beta_in, BX, mate).start()
        alpha_last[...] = jnp.ones_like(alpha_last)
        alpha_in_value = jnp.ones((piece, LANES), jnp.float32)

        @when(first_g)
        def _():
            alpha_in[...] = alpha_in_value

        @when(no(first_g))
        def _():
            received(alpha_in, AX)
            received(f1_in, F1)
            a, s = sum_pieces(f1_in)
            alpha_last[...] = a * (states / s)

        copy(alpha_last, alpha_last, AO, mate).start()
        wait_up()

        @when(no(last_g))
        def _():
            scaling = target / (alpha_in[...] * beta[...])
            forward(scaling * alpha_last[...], high, lambda i: to_group(f_out.at[i], f1_in, F1, g + 1, i))

        received(beta_last, BO)

    result = target / (alpha_last[...] * beta_last[...])
    out[...] = jnp.where(lead, result[piece // CORES :], result[: piece // CORES])

    sent(row_in, RX)
    sent(marg.at[core], MX)
    sent(half, KX)

    @when(lead)
    def _():
        sent(beta_last, BO)

        @when(no(up_collector))
        def _():
            sent(col_out, CS)

        @when(up_collector)
        def _():
            sent(many, CB)

            @when(first_g)
            def _():
                sent(col_in, A1)

        @when(both(g > 0, no(last_g)))
        def _():
            sent(f0_in, F0)

        @when(no(first_g))
        def _():
            sent(alpha, AX)
            sent(w1_in, W1)

        @when(both(last_g, no(up_collector)))
        def _():
            sent(f_out, AR)

        @when(both(last_g, up_collector))
        def _():
            sent(many.at[pl.ds(0, chips - 1)], LS)

    @when(no(lead))
    def _():
        sent(col_out, PK)
        sent(beta, BX)
        sent(alpha_last, AO)

        @when(no(first_g))
        def _():
            sent(b0_in, B0)

        @when(no(last_g))
        def _():
            sent(f1_in, F1)


def solution(mesh):
    chain = mesh.shape["chain"]

    def on_device(cost, marginals, final_marginal):
        rows, states = cost.shape
        width = states // rows
        chips = width // CORES
        own = rows // LANES
        piece = CORES * own

        def buffer(*shape):
            return pltpu.VMEM(shape + (LANES,), jnp.float32)

        one = buffer(piece)
        whole = buffer(chips, piece)
        pieces = buffer(chips, piece + 1)
        scratch = dict(
            kernel=pltpu.VMEM((CORES * rows, states), jnp.float32), column=buffer(CORES * rows),
            marg=buffer(CORES, own), fin=whole, row_out=buffer(own), row_in=buffer(own), rsum=one,
            col_out=whole, col_mate=whole, col_in=whole, cs_in=buffer(chips, chips, piece),
            many=buffer(width - 1, chips, piece),
            a1_in=one, f_out=pieces, f0_in=pieces, f1_in=pieces, ar_in=buffer(chips, chips, piece + 1),
            b0_out=buffer(piece + 1), b0_in=pieces, w0=whole, w1_out=whole, w1_in=whole,
            alpha=one, alpha_in=one, beta=one, beta_in=one, alpha_last=one, beta_last=one,
            load_sem=pltpu.SemaphoreType.DMA((CHUNKS + 2,)), send_sem=pltpu.SemaphoreType.DMA((len(SLOTS),)),
            recv_sem=pltpu.SemaphoreType.DMA((len(SLOTS),)), token=pltpu.SemaphoreType.REGULAR((2,)),
        )
        scaling = pl.pallas_call(
            functools.partial(chain_kernel, width, chain // width),
            out_shape=jax.ShapeDtypeStruct((own, LANES), jnp.float32),
            in_specs=[pl.BlockSpec(memory_space=pl.ANY)] * 3,
            out_specs=pl.BlockSpec(memory_space=pltpu.VMEM),
            scratch_shapes=scratch,
            compiler_params=pltpu.CompilerParams(collective_id=0, has_side_effects=True),
            name="sinkhorn_chain",
        )(cost, marginals.reshape(own, LANES), final_marginal.reshape(chips, piece, LANES))
        return jnp.log(scaling).reshape(rows)

    placed = (P(("pop", "chain"), None), P(("pop", "chain")), P("pop"))
    return jax.shard_map(on_device, mesh=mesh, in_specs=placed, out_specs=P(("pop", "chain")), check_vma=False)
```

```python
import functools
import math

import jax
import jax.numpy as jnp
from jax import lax
from jax.experimental import pallas as pl
from jax.experimental.pallas import tpu as pltpu
from jax.sharding import PartitionSpec as P

ENTROPIC = 0.25
LANES = 128
SUBLANES = 8
CHUNKS = 8
CORES = 2
QUARTERS = 4
MESH = pl.DeviceIdType.MESH
SLOTS = range(16)
KX, RX, MX, CS, CB, A1, F0, AR, LS, B0, W1, F1, AX, BX, AO, BO = SLOTS


def eye():
    shape = (LANES, LANES)
    return lax.broadcasted_iota(jnp.int32, shape, 0) == lax.broadcasted_iota(jnp.int32, shape, 1)


def total(x):
    return jnp.sum(jnp.sum(x, axis=0, keepdims=True), axis=1, keepdims=True)


def tree(values):
    while len(values) > 1:
        values = [a + b for a, b in zip(values[::2], values[1::2])] + values[len(values) // 2 * 2 :]
    return values[0]


def signal(sem, target):
    pl.semaphore_signal(sem, inc=1, device_id={"chain": target}, device_id_type=MESH)


def chain_kernel(
    width, kernels, cost, marginals, final, out,
    kernel, column, marg, fin, row_out, row_in, rsum, col_out, col_in, cs_in, many,
    a1_in, f_out, f0_in, f1_in, ar_in, b0_out, b0_in, w0, w1_out, w1_in,
    alpha, alpha_in, beta, beta_in, alpha_last, beta_last,
    load_sem, send_sem, recv_sem, token,
):
    states = kernel.shape[1]
    rows = kernel.shape[0] // CORES
    blocks = states // LANES
    piece = kernel.shape[0] // LANES
    own = piece // CORES
    chips = width // CORES
    me = lax.axis_index("chain")
    g = me // width
    m = me % width
    chip = m // CORES
    core = m % CORES
    mate = me + 1 - 2 * core
    start = g * width
    first_g, last_g = g == 0, g == kernels - 1
    lead = core == 1
    up_collector = jnp.logical_and(lead, chip == chips - 1)
    down_collector = jnp.logical_and(lead, chip == 0)
    owner = start + width - 1

    def when(condition):
        return pl.when(condition)

    def both(*conditions):
        return functools.reduce(jnp.logical_and, conditions)

    def no(condition):
        return jnp.logical_not(condition)

    def copy(src, dst, slot, target):
        return pltpu.make_async_remote_copy(
            src_ref=src, dst_ref=dst, send_sem=send_sem.at[slot], recv_sem=recv_sem.at[slot],
            device_id={"chain": target}, device_id_type=MESH,
        )

    def received(ref, slot):
        copy(ref, ref, slot, mate).wait_recv()

    def sent(ref, slot):
        copy(ref, ref, slot, mate).wait_send()

    barrier = pltpu.get_barrier_semaphore()
    signal(barrier, mate)

    @when(both(me != owner, mate != owner))
    def _():
        signal(barrier, owner)

    @when(both(me != start + 1, mate != start + 1))
    def _():
        signal(barrier, start + 1)

    @when(no(first_g))
    def _():
        signal(barrier, owner - width)

    @when(no(last_g))
    def _():
        signal(barrier, start + width + 1)

    @when(up_collector)
    def _():
        for i in range(width - CORES):
            if i != 1:
                signal(barrier, start + i)

    span = rows // CHUNKS
    base = core * rows

    def load(c):
        return pltpu.make_async_copy(
            cost.at[pl.ds(c * span, span)], kernel.at[pl.ds(base + c * span, span)], load_sem.at[c]
        )

    for c in range(CHUNKS):
        load(c).start()
    marg_load = pltpu.make_async_copy(marginals, marg.at[core], load_sem.at[CHUNKS])
    fin_load = pltpu.make_async_copy(final, fin, load_sem.at[CHUNKS + 1])
    marg_load.start()
    fin_load.start()

    def lanes(b):
        return slice(b * LANES, (b + 1) * LANES)

    def row_of_column(ref, first, count):
        parts = []
        for h in range(first, first + count):
            x = jnp.sum(ref[h * LANES : (h + 1) * LANES, :], axis=1, keepdims=True)
            parts.append(jnp.sum(jnp.where(eye(), x, 0.0), axis=0, keepdims=True))
        return jnp.concatenate(parts, axis=0)

    def column_of_row(value):
        for h in range(piece):
            x = jnp.broadcast_to(value[h : h + 1, :], (LANES, LANES))
            x = jnp.sum(jnp.where(eye(), x, 0.0), axis=1, keepdims=True)
            column[h * LANES : (h + 1) * LANES, :] = jnp.broadcast_to(x, (LANES, LANES))

    def forward(v, order, send):
        column_of_row(v)
        row = jnp.sum(v * rsum[...], axis=0, keepdims=True)
        quarters = min(QUARTERS, chips)
        for q in range(quarters):
            targets = order[q * chips // quarters : (q + 1) * chips // quarters]
            mine = [i * piece + h for i in targets for h in range(piece)]

            def step(r, acc):
                at = pl.ds(pl.multiple_of(r * SUBLANES, SUBLANES), SUBLANES)
                v = column[at, :]
                return tuple(a + kernel[at, lanes(b)] * v for a, b in zip(acc, mine))

            zero = tuple(jnp.zeros((SUBLANES, LANES), jnp.float32) for _ in mine)
            acc = lax.fori_loop(0, CORES * rows // SUBLANES, step, zero, unroll=8)
            for n, i in enumerate(targets):
                for h in range(piece):
                    f_out[i, h : h + 1, :] = jnp.sum(acc[n * piece + h], axis=0, keepdims=True)
                f_out[i, piece : piece + 1, :] = row
            for i in targets:
                send(i)

    def backward(w, emit):
        ws = [jnp.broadcast_to(w(b), (SUBLANES, LANES)) for b in range(blocks)]

        def step(r, carry):
            at = pl.ds(pl.multiple_of(r * SUBLANES, SUBLANES), SUBLANES)
            x = [kernel[at, lanes(b)] * ws[b] for b in range(4)]
            for b in range(4, blocks):
                x[b % 4] = x[b % 4] + kernel[at, lanes(b)] * ws[b]
            column[at, :] = tree(x)
            return carry

        for h in range(CORES):
            lax.fori_loop(h * rows // SUBLANES, (h + 1) * rows // SUBLANES, step, 0, unroll=8)
            emit(h, row_of_column(column, h * own, own))

    def sum_pieces(ref):
        x = tree([ref[i] for i in range(chips)])
        return x[:piece], total(x[piece:])

    rate = -math.log2(math.e) / ENTROPIC

    def chunk_step(r, acc):
        at = pl.ds(pl.multiple_of(base + r * SUBLANES, SUBLANES), SUBLANES)
        new, xs = [], []
        for b in range(blocks):
            x = jnp.exp2(kernel[at, lanes(b)] * rate)
            kernel[at, lanes(b)] = x
            xs.append(x)
            new.append(acc[b] + x)
        here = pl.ds(pl.multiple_of(r * SUBLANES, SUBLANES), SUBLANES)
        column[here, :] = tree(xs)
        return tuple(new)

    acc = tuple(jnp.zeros((SUBLANES, LANES), jnp.float32) for _ in range(blocks))
    for c in range(CHUNKS):
        load(c).wait()
        acc = lax.fori_loop(c * span // SUBLANES, (c + 1) * span // SUBLANES, chunk_step, acc)
    for b in range(blocks):
        col_out[b // piece, b % piece : b % piece + 1, :] = jnp.sum(acc[b], axis=0, keepdims=True)
    row_out[...] = row_of_column(column, 0, own)
    marg_load.wait()
    fin_load.wait()

    greeted = jnp.where(mate == owner, 1, 2)
    greeted = jnp.where(down_collector, width - 1 + jnp.where(first_g, 0, width), greeted)
    greeted = jnp.where(up_collector, width - 1 + jnp.where(last_g, 0, width), greeted)
    pl.semaphore_wait(barrier, greeted)

    UP, DOWN = 0, 1

    @when(both(up_collector, no(last_g)))
    def _():
        for i in range(width - 1):
            signal(token.at[UP], start + i)

    @when(both(down_collector, no(first_g)))
    def _():
        for i in range(width):
            if i != 1:
                signal(token.at[DOWN], start + i)

    @when(no(up_collector))
    def _():
        copy(col_out, cs_in.at[m], CS, owner).start()

    copy(row_out, row_in, RX, mate).start()
    copy(marg.at[core], marg.at[core], MX, mate).start()
    half = kernel.at[pl.ds(base, rows)]
    copy(half, half, KX, mate).start()

    def wait_up():
        @when(both(no(up_collector), no(last_g)))
        def _():
            pl.semaphore_wait(token.at[UP], 1)

    def wait_down():
        @when(both(no(down_collector), no(first_g)))
        def _():
            pl.semaphore_wait(token.at[DOWN], 1)

    def to_group(src, dst, slot, group, i):
        copy(src, dst.at[chip], slot, group * width + CORES * i + core).start()

    high = list(range(chips - 1, -1, -1))
    low = list(range(chips))

    @when(up_collector)
    def _():
        cs_in[width - 1] = col_out[...]
        received(cs_in.at[pl.ds(0, width - 1)], CS)
        c = tree([cs_in[i] for i in range(width)])
        col_in[...] = c

        @when(first_g)
        def _():
            w0[...] = c * (states / total(jnp.sum(c, axis=0)))
            for i in high:
                copy(w0.at[i], a1_in, A1, start + width + CORES * i + 1).start()

        for i in range(width - 1):
            copy(col_in, col_in, CB, start + i).start()

    received(row_in, RX)

    @when(lead)
    def _():
        rsum[...] = jnp.concatenate([row_in[...], row_out[...]], axis=0)

    @when(no(lead))
    def _():
        rsum[...] = jnp.concatenate([row_out[...], row_in[...]], axis=0)

    received(marg.at[1 - core], MX)
    target = jnp.concatenate([marg[i] for i in range(CORES)], axis=0)

    def factor(products):
        return states / total(jnp.sum(products, axis=0))

    @when(lead)
    def _():
        alpha[...] = jnp.ones_like(alpha)

        @when(g == 1)
        def _():
            received(a1_in, A1)
            alpha[...] = a1_in[...]

        @when(g > 1)
        def _():
            received(f0_in, F0)
            a, s = sum_pieces(f0_in)
            alpha[...] = a * (states / s)

        received(kernel.at[pl.ds(0, rows)], KX)
        wait_up()

        @when(no(first_g))
        def _():
            def send(i):
                @when(no(last_g))
                def _():
                    to_group(f_out.at[i], f0_in, F0, g + 1, i)

                @when(both(last_g, no(up_collector)))
                def _():
                    copy(f_out.at[i], ar_in.at[chip, i], AR, owner).start()

            forward(alpha[...], high, send)
            copy(alpha, alpha_in, AX, mate).start()

        @when(both(last_g, no(up_collector)))
        def _():
            received(w1_in, LS)

        @when(both(last_g, up_collector))
        def _():
            ar_in[chips - 1] = f_out[...]
            received(ar_in.at[pl.ds(0, chips - 1)], AR)
            x = tree([ar_in[i] for i in range(chips)])[:, :piece]
            x = fin[...] / (x * (states / total(jnp.sum(x, axis=0))))
            for h in range(CORES):
                w1_in[h] = x[:, h * own : (h + 1) * own]
            for i in range(chips - 1):
                copy(w1_in, w1_in, LS, start + CORES * i + 1).start()

        @when(no(up_collector))
        def _():
            received(col_in, CB)

        received(beta_in, BX)
        scaling = target / (alpha[...] * beta_in[...])

        @when(no(last_g))
        def _():
            received(w1_in, W1)

        wait_down()

        def send_w(h, b):
            f = factor(sum(col_in[:, k * own : (k + 1) * own, :] * w1_in[k] for k in range(CORES)))
            b = b * f
            beta_last[h * own : (h + 1) * own, :] = b

            @when(no(first_g))
            def _():
                w1_out[h, 0] = scaling[h * own : (h + 1) * own] * b
                for i in low:
                    copy(w1_out.at[h, 0], w1_in.at[h, chip], W1, start - width + CORES * i + core).start()

        backward(lambda b: w1_in[b % piece // own, b // piece, b % own : b % own + 1, :], send_w)
        copy(beta_last, beta_last, BO, mate).start()
        received(alpha_last, AO)

    @when(no(lead))
    def _():
        def send_b(b):
            b0_out[0:piece, :] = b
            b0_out[piece : piece + 1, :] = jnp.sum(b, axis=0, keepdims=True)
            wait_down()
            for i in low:
                to_group(b0_out, b0_in, B0, g - 1, i)

        @when(last_g)
        def _():
            send_b(rsum[...])
            received(col_in, CB)
            beta[...] = rsum[...] * factor(col_in[...])

        received(kernel.at[pl.ds(rows, rows)], KX)

        @when(no(last_g))
        def _():
            received(b0_in, B0)
            x = b0_in[...]
            s = total(tree([x[i, piece:] for i in range(chips)]))
            w0[...] = x[:, :piece] * (states / s)

            def keep(h, b):
                beta[h * own : (h + 1) * own, :] = b

            backward(lambda b: w0[b // piece, b % piece : b % piece + 1, :], keep)

            @when(no(first_g))
            def _():
                send_b(beta[...])

            received(col_in, CB)
            beta[...] = beta[...] * factor(col_in[...] * w0[...])

        copy(beta, beta_in, BX, mate).start()
        alpha_last[...] = jnp.ones_like(alpha_last)
        alpha_in_value = jnp.ones((piece, LANES), jnp.float32)

        @when(first_g)
        def _():
            alpha_in[...] = alpha_in_value

        @when(no(first_g))
        def _():
            received(alpha_in, AX)
            received(f1_in, F1)
            a, s = sum_pieces(f1_in)
            alpha_last[...] = a * (states / s)

        copy(alpha_last, alpha_last, AO, mate).start()
        wait_up()

        @when(no(last_g))
        def _():
            scaling = target / (alpha_in[...] * beta[...])
            forward(scaling * alpha_last[...], high, lambda i: to_group(f_out.at[i], f1_in, F1, g + 1, i))

        received(beta_last, BO)

    result = target / (alpha_last[...] * beta_last[...])
    out[...] = jnp.where(lead, result[own:], result[:own])

    sent(row_in, RX)
    sent(marg.at[core], MX)
    sent(half, KX)

    @when(no(up_collector))
    def _():
        sent(col_out, CS)

    @when(lead)
    def _():
        sent(beta_last, BO)

        @when(up_collector)
        def _():
            sent(many, CB)

            @when(first_g)
            def _():
                sent(col_in, A1)

        @when(both(g > 0, no(last_g)))
        def _():
            sent(f0_in, F0)

        @when(no(first_g))
        def _():
            sent(alpha, AX)
            sent(w1_in, W1)

        @when(both(last_g, no(up_collector)))
        def _():
            sent(f_out, AR)

        @when(both(last_g, up_collector))
        def _():
            sent(many.at[pl.ds(0, chips - 1)], LS)

    @when(no(lead))
    def _():
        sent(beta, BX)
        sent(alpha_last, AO)

        @when(no(first_g))
        def _():
            sent(b0_in, B0)

        @when(no(last_g))
        def _():
            sent(f1_in, F1)


def solution(mesh):
    chain = mesh.shape["chain"]

    def on_device(cost, marginals, final_marginal):
        rows, states = cost.shape
        width = states // rows
        chips = width // CORES
        own = rows // LANES
        piece = CORES * own

        def buffer(*shape):
            return pltpu.VMEM(shape + (LANES,), jnp.float32)

        one = buffer(piece)
        whole = buffer(chips, piece)
        pieces = buffer(chips, piece + 1)
        scratch = dict(
            kernel=pltpu.VMEM((CORES * rows, states), jnp.float32), column=buffer(CORES * rows),
            marg=buffer(CORES, own), fin=whole, row_out=buffer(own), row_in=buffer(own), rsum=one,
            col_out=whole, col_in=whole, cs_in=buffer(width, chips, piece),
            many=buffer(width - 1, chips, piece),
            a1_in=one, f_out=pieces, f0_in=pieces, f1_in=pieces, ar_in=buffer(chips, chips, piece + 1),
            b0_out=buffer(piece + 1), b0_in=pieces, w0=whole, w1_out=buffer(CORES, chips, own), w1_in=buffer(CORES, chips, own),
            alpha=one, alpha_in=one, beta=one, beta_in=one, alpha_last=one, beta_last=one,
            load_sem=pltpu.SemaphoreType.DMA((CHUNKS + 2,)), send_sem=pltpu.SemaphoreType.DMA((len(SLOTS),)),
            recv_sem=pltpu.SemaphoreType.DMA((len(SLOTS),)), token=pltpu.SemaphoreType.REGULAR((2,)),
        )
        scaling = pl.pallas_call(
            functools.partial(chain_kernel, width, chain // width),
            out_shape=jax.ShapeDtypeStruct((own, LANES), jnp.float32),
            in_specs=[pl.BlockSpec(memory_space=pl.ANY)] * 3,
            out_specs=pl.BlockSpec(memory_space=pltpu.VMEM),
            scratch_shapes=scratch,
            compiler_params=pltpu.CompilerParams(collective_id=0, has_side_effects=True),
            name="sinkhorn_chain",
        )(cost, marginals.reshape(own, LANES), final_marginal.reshape(chips, piece, LANES))
        return jnp.log(scaling).reshape(rows)

    placed = (P(("pop", "chain"), None), P(("pop", "chain")), P("pop"))
    return jax.shard_map(on_device, mesh=mesh, in_specs=placed, out_specs=P(("pop", "chain")), check_vma=False)
```

```python
import functools
import math

import jax
import jax.numpy as jnp
from jax import lax
from jax.experimental import pallas as pl
from jax.experimental.pallas import tpu as pltpu
from jax.sharding import PartitionSpec as P

ENTROPIC = 0.25
LANES = 128
SUBLANES = 8
CHUNKS = 8
CORES = 2
QUARTERS = 4
MESH = pl.DeviceIdType.MESH
SLOTS = range(16)
KX, RX, MX, CS, CB, A1, F0, AR, LS, B0, W1, F1, AX, BX, AO, BO = SLOTS


def eye():
    shape = (LANES, LANES)
    return lax.broadcasted_iota(jnp.int32, shape, 0) == lax.broadcasted_iota(jnp.int32, shape, 1)


def total(x):
    return jnp.sum(jnp.sum(x, axis=0, keepdims=True), axis=1, keepdims=True)


def tree(values):
    while len(values) > 1:
        values = [a + b for a, b in zip(values[::2], values[1::2])] + values[len(values) // 2 * 2 :]
    return values[0]


def signal(sem, target):
    pl.semaphore_signal(sem, inc=1, device_id={"chain": target}, device_id_type=MESH)


def chain_kernel(
    width, kernels, cost, marginals, final, out,
    kernel, column, marg, fin, row_out, row_in, rsum, col_out, col_in, cs_in, many,
    a1_in, f_out, f0_in, f1_in, ar_in, b0_out, b0_in, w0, w1_out, w1_in,
    alpha, alpha_in, beta, beta_in, alpha_last, beta_last,
    load_sem, send_sem, recv_sem, token,
):
    states = kernel.shape[1]
    rows = kernel.shape[0] // CORES
    blocks = states // LANES
    piece = kernel.shape[0] // LANES
    own = piece // CORES
    chips = width // CORES
    me = lax.axis_index("chain")
    g = me // width
    m = me % width
    chip = m // CORES
    core = m % CORES
    mate = me + 1 - 2 * core
    start = g * width
    first_g, last_g = g == 0, g == kernels - 1
    lead = core == 1
    up_collector = jnp.logical_and(lead, chip == chips - 1)
    down_collector = jnp.logical_and(lead, chip == 0)
    owner = start + width - 1

    def when(condition):
        return pl.when(condition)

    def both(*conditions):
        return functools.reduce(jnp.logical_and, conditions)

    def no(condition):
        return jnp.logical_not(condition)

    def copy(src, dst, slot, target):
        return pltpu.make_async_remote_copy(
            src_ref=src, dst_ref=dst, send_sem=send_sem.at[slot], recv_sem=recv_sem.at[slot],
            device_id={"chain": target}, device_id_type=MESH,
        )

    def received(ref, slot):
        copy(ref, ref, slot, mate).wait_recv()

    def sent(ref, slot):
        copy(ref, ref, slot, mate).wait_send()

    span = rows // CHUNKS
    base = core * rows

    def load(c):
        return pltpu.make_async_copy(
            cost.at[pl.ds(c * span, span)], kernel.at[pl.ds(base + c * span, span)], load_sem.at[c]
        )

    for c in range(CHUNKS):
        load(c).start()
    marg_load = pltpu.make_async_copy(marginals, marg.at[core], load_sem.at[CHUNKS])
    fin_load = pltpu.make_async_copy(final, fin, load_sem.at[CHUNKS + 1])
    marg_load.start()
    fin_load.start()

    barrier = pltpu.get_barrier_semaphore()
    signal(barrier, mate)

    @when(both(me != owner, mate != owner))
    def _():
        signal(barrier, owner)

    @when(both(me != start + 1, mate != start + 1))
    def _():
        signal(barrier, start + 1)

    @when(no(first_g))
    def _():
        signal(barrier, owner - width)

    @when(no(last_g))
    def _():
        signal(barrier, start + width + 1)

    @when(up_collector)
    def _():
        for i in range(width - CORES):
            if i != 1:
                signal(barrier, start + i)

    def lanes(b):
        return slice(b * LANES, (b + 1) * LANES)

    def row_of_column(ref, first, count):
        parts = []
        for h in range(first, first + count):
            x = jnp.sum(ref[h * LANES : (h + 1) * LANES, :], axis=1, keepdims=True)
            parts.append(jnp.sum(jnp.where(eye(), x, 0.0), axis=0, keepdims=True))
        return jnp.concatenate(parts, axis=0)

    def column_of_row(value):
        for h in range(piece):
            x = jnp.broadcast_to(value[h : h + 1, :], (LANES, LANES))
            x = jnp.sum(jnp.where(eye(), x, 0.0), axis=1, keepdims=True)
            column[h * LANES : (h + 1) * LANES, :] = jnp.broadcast_to(x, (LANES, LANES))

    def forward(v, order, send):
        column_of_row(v)
        row = jnp.sum(v * rsum[...], axis=0, keepdims=True)
        quarters = min(QUARTERS, chips)
        for q in range(quarters):
            targets = order[q * chips // quarters : (q + 1) * chips // quarters]
            mine = [i * piece + h for i in targets for h in range(piece)]

            def step(r, acc):
                at = pl.ds(pl.multiple_of(r * SUBLANES, SUBLANES), SUBLANES)
                v = column[at, :]
                return tuple(a + kernel[at, lanes(b)] * v for a, b in zip(acc, mine))

            zero = tuple(jnp.zeros((SUBLANES, LANES), jnp.float32) for _ in mine)
            acc = lax.fori_loop(0, CORES * rows // SUBLANES, step, zero, unroll=8)
            for n, i in enumerate(targets):
                for h in range(piece):
                    f_out[i, h : h + 1, :] = jnp.sum(acc[n * piece + h], axis=0, keepdims=True)
                f_out[i, piece : piece + 1, :] = row
            for i in targets:
                send(i)

    def backward(w, emit):
        ws = [jnp.broadcast_to(w(b), (SUBLANES, LANES)) for b in range(blocks)]

        def step(r, carry):
            at = pl.ds(pl.multiple_of(r * SUBLANES, SUBLANES), SUBLANES)
            x = [kernel[at, lanes(b)] * ws[b] for b in range(4)]
            for b in range(4, blocks):
                x[b % 4] = x[b % 4] + kernel[at, lanes(b)] * ws[b]
            column[at, :] = tree(x)
            return carry

        for h in range(CORES):
            lax.fori_loop(h * rows // SUBLANES, (h + 1) * rows // SUBLANES, step, 0, unroll=8)
            emit(h, row_of_column(column, h * own, own))

    def sum_pieces(ref):
        x = tree([ref[i] for i in range(chips)])
        return x[:piece], total(x[piece:])

    rate = -math.log2(math.e) / ENTROPIC

    def chunk_step(r, acc):
        at = pl.ds(pl.multiple_of(base + r * SUBLANES, SUBLANES), SUBLANES)
        new, xs = [], []
        for b in range(blocks):
            x = jnp.exp2(kernel[at, lanes(b)] * rate)
            kernel[at, lanes(b)] = x
            xs.append(x)
            new.append(acc[b] + x)
        here = pl.ds(pl.multiple_of(r * SUBLANES, SUBLANES), SUBLANES)
        column[here, :] = tree(xs)
        return tuple(new)

    acc = tuple(jnp.zeros((SUBLANES, LANES), jnp.float32) for _ in range(blocks))
    for c in range(CHUNKS):
        load(c).wait()
        acc = lax.fori_loop(c * span // SUBLANES, (c + 1) * span // SUBLANES, chunk_step, acc)
    for b in range(blocks):
        col_out[b // piece, b % piece : b % piece + 1, :] = jnp.sum(acc[b], axis=0, keepdims=True)

    greeted = jnp.where(mate == owner, 1, 2)
    greeted = jnp.where(down_collector, width - 1 + jnp.where(first_g, 0, width), greeted)
    greeted = jnp.where(up_collector, width - 1 + jnp.where(last_g, 0, width), greeted)
    pl.semaphore_wait(barrier, greeted)

    UP, DOWN = 0, 1

    @when(both(up_collector, no(last_g)))
    def _():
        for i in range(width - 1):
            signal(token.at[UP], start + i)

    @when(both(down_collector, no(first_g)))
    def _():
        for i in range(width):
            if i != 1:
                signal(token.at[DOWN], start + i)

    @when(no(up_collector))
    def _():
        copy(col_out, cs_in.at[m], CS, owner).start()

    row_out[...] = row_of_column(column, 0, own)
    marg_load.wait()
    fin_load.wait()
    copy(row_out, row_in, RX, mate).start()
    copy(marg.at[core], marg.at[core], MX, mate).start()
    half = kernel.at[pl.ds(base, rows)]
    copy(half, half, KX, mate).start()

    def wait_up():
        @when(both(no(up_collector), no(last_g)))
        def _():
            pl.semaphore_wait(token.at[UP], 1)

    def wait_down():
        @when(both(no(down_collector), no(first_g)))
        def _():
            pl.semaphore_wait(token.at[DOWN], 1)

    def to_group(src, dst, slot, group, i):
        copy(src, dst.at[chip], slot, group * width + CORES * i + core).start()

    high = list(range(chips - 1, -1, -1))
    low = list(range(chips))

    @when(up_collector)
    def _():
        cs_in[width - 1] = col_out[...]
        received(cs_in.at[pl.ds(0, width - 1)], CS)
        c = tree([cs_in[i] for i in range(width)])
        col_in[...] = c

        @when(first_g)
        def _():
            w0[...] = c * (states / total(jnp.sum(c, axis=0)))
            for i in high:
                copy(w0.at[i], a1_in, A1, start + width + CORES * i + 1).start()

        for i in range(width - 1):
            copy(col_in, col_in, CB, start + i).start()

    received(row_in, RX)

    @when(lead)
    def _():
        rsum[...] = jnp.concatenate([row_in[...], row_out[...]], axis=0)

    @when(no(lead))
    def _():
        rsum[...] = jnp.concatenate([row_out[...], row_in[...]], axis=0)

    received(marg.at[1 - core], MX)
    target = jnp.concatenate([marg[i] for i in range(CORES)], axis=0)

    def factor(products):
        return states / total(jnp.sum(products, axis=0))

    @when(lead)
    def _():
        alpha[...] = jnp.ones_like(alpha)

        @when(g == 1)
        def _():
            received(a1_in, A1)
            alpha[...] = a1_in[...]

        @when(g > 1)
        def _():
            received(f0_in, F0)
            a, s = sum_pieces(f0_in)
            alpha[...] = a * (states / s)

        received(kernel.at[pl.ds(0, rows)], KX)
        wait_up()

        @when(no(first_g))
        def _():
            def send(i):
                @when(no(last_g))
                def _():
                    to_group(f_out.at[i], f0_in, F0, g + 1, i)

                @when(both(last_g, no(up_collector)))
                def _():
                    copy(f_out.at[i, pl.ds(0, piece)], ar_in.at[chip, i], AR, owner).start()

            forward(alpha[...], high, send)
            copy(alpha, alpha_in, AX, mate).start()

        @when(both(last_g, no(up_collector)))
        def _():
            received(w1_in, LS)

        @when(both(last_g, up_collector))
        def _():
            ar_in[chips - 1] = f_out[:, :piece, :]
            received(ar_in.at[pl.ds(0, chips - 1)], AR)
            x = tree([ar_in[i] for i in range(chips)])
            x = fin[...] / (x * (states / total(jnp.sum(x, axis=0))))
            for h in range(CORES):
                w1_in[h] = x[:, h * own : (h + 1) * own]
            for i in range(chips - 1):
                copy(w1_in, w1_in, LS, start + CORES * i + 1).start()

        @when(no(up_collector))
        def _():
            received(col_in, CB)

        received(beta_in, BX)
        scaling = target / (alpha[...] * beta_in[...])

        @when(no(last_g))
        def _():
            received(w1_in, W1)

        wait_down()

        def send_w(h, b):
            f = factor(sum(col_in[:, k * own : (k + 1) * own, :] * w1_in[k] for k in range(CORES)))
            b = b * f
            beta_last[h] = b
            if h == 0:
                copy(beta_last.at[0], beta_last.at[0], BO, mate).start()

            @when(no(first_g))
            def _():
                w1_out[h, 0] = scaling[h * own : (h + 1) * own] * b
                for i in low:
                    copy(w1_out.at[h, 0], w1_in.at[h, chip], W1, start - width + CORES * i + core).start()

        backward(lambda b: w1_in[b % piece // own, b // piece, b % own : b % own + 1, :], send_w)
        received(alpha_last, AO)
        out[...] = target[own:] / (alpha_last[own:, :] * beta_last[1])

    @when(no(lead))
    def _():
        def send_b(b):
            b0_out[0:piece, :] = b
            b0_out[piece : piece + 1, :] = jnp.sum(b, axis=0, keepdims=True)
            wait_down()
            for i in low:
                to_group(b0_out, b0_in, B0, g - 1, i)

        @when(last_g)
        def _():
            send_b(rsum[...])
            received(col_in, CB)
            beta[...] = rsum[...] * factor(col_in[...])

        received(kernel.at[pl.ds(rows, rows)], KX)

        @when(no(last_g))
        def _():
            received(b0_in, B0)
            x = b0_in[...]
            s = total(tree([x[i, piece:] for i in range(chips)]))
            w0[...] = x[:, :piece] * (states / s)

            def keep(h, b):
                beta[h * own : (h + 1) * own, :] = b

            backward(lambda b: w0[b // piece, b % piece : b % piece + 1, :], keep)

            @when(no(first_g))
            def _():
                send_b(beta[...])

            received(col_in, CB)
            beta[...] = beta[...] * factor(col_in[...] * w0[...])

        copy(beta, beta_in, BX, mate).start()
        alpha_last[...] = jnp.ones_like(alpha_last)
        alpha_in_value = jnp.ones((piece, LANES), jnp.float32)

        @when(first_g)
        def _():
            alpha_in[...] = alpha_in_value

        @when(no(first_g))
        def _():
            received(alpha_in, AX)
            received(f1_in, F1)
            a, s = sum_pieces(f1_in)
            alpha_last[...] = a * (states / s)

        copy(alpha_last, alpha_last, AO, mate).start()
        wait_up()

        @when(no(last_g))
        def _():
            scaling = target / (alpha_in[...] * beta[...])
            forward(scaling * alpha_last[...], high, lambda i: to_group(f_out.at[i], f1_in, F1, g + 1, i))

        received(beta_last.at[0], BO)
        out[...] = target[:own] / (alpha_last[:own, :] * beta_last[0])

    sent(row_in, RX)
    sent(marg.at[core], MX)
    sent(half, KX)

    @when(no(up_collector))
    def _():
        sent(col_out, CS)

    @when(lead)
    def _():
        sent(beta_last.at[0], BO)

        @when(up_collector)
        def _():
            sent(many, CB)

            @when(first_g)
            def _():
                sent(col_in, A1)

        @when(both(g > 0, no(last_g)))
        def _():
            sent(f0_in, F0)

        @when(no(first_g))
        def _():
            sent(alpha, AX)
            sent(w1_in, W1)

        @when(both(last_g, no(up_collector)))
        def _():
            sent(w0, AR)

        @when(both(last_g, up_collector))
        def _():
            sent(many.at[pl.ds(0, chips - 1)], LS)

    @when(no(lead))
    def _():
        sent(beta, BX)
        sent(alpha_last, AO)

        @when(no(first_g))
        def _():
            sent(b0_in, B0)

        @when(no(last_g))
        def _():
            sent(f1_in, F1)


def solution(mesh):
    chain = mesh.shape["chain"]

    def on_device(cost, marginals, final_marginal):
        rows, states = cost.shape
        width = states // rows
        chips = width // CORES
        own = rows // LANES
        piece = CORES * own

        def buffer(*shape):
            return pltpu.VMEM(shape + (LANES,), jnp.float32)

        one = buffer(piece)
        whole = buffer(chips, piece)
        pieces = buffer(chips, piece + 1)
        scratch = dict(
            kernel=pltpu.VMEM((CORES * rows, states), jnp.float32), column=buffer(CORES * rows),
            marg=buffer(CORES, own), fin=whole, row_out=buffer(own), row_in=buffer(own), rsum=one,
            col_out=whole, col_in=whole, cs_in=buffer(width, chips, piece),
            many=buffer(width - 1, chips, piece),
            a1_in=one, f_out=pieces, f0_in=pieces, f1_in=pieces, ar_in=buffer(chips, chips, piece),
            b0_out=buffer(piece + 1), b0_in=pieces, w0=whole, w1_out=buffer(CORES, chips, own), w1_in=buffer(CORES, chips, own),
            alpha=one, alpha_in=one, beta=one, beta_in=one, alpha_last=one, beta_last=buffer(CORES, own),
            load_sem=pltpu.SemaphoreType.DMA((CHUNKS + 2,)), send_sem=pltpu.SemaphoreType.DMA((len(SLOTS),)),
            recv_sem=pltpu.SemaphoreType.DMA((len(SLOTS),)), token=pltpu.SemaphoreType.REGULAR((2,)),
        )
        scaling = pl.pallas_call(
            functools.partial(chain_kernel, width, chain // width),
            out_shape=jax.ShapeDtypeStruct((own, LANES), jnp.float32),
            in_specs=[pl.BlockSpec(memory_space=pl.ANY)] * 3,
            out_specs=pl.BlockSpec(memory_space=pltpu.VMEM),
            scratch_shapes=scratch,
            compiler_params=pltpu.CompilerParams(collective_id=0, has_side_effects=True),
            name="sinkhorn_chain",
        )(cost, marginals.reshape(own, LANES), final_marginal.reshape(chips, piece, LANES))
        return jnp.log(scaling).reshape(rows)

    placed = (P(("pop", "chain"), None), P(("pop", "chain")), P("pop"))
    return jax.shard_map(on_device, mesh=mesh, in_specs=placed, out_specs=P(("pop", "chain")), check_vma=False)
```

```python
import functools
import math

import jax
import jax.numpy as jnp
from jax import lax
from jax.experimental import pallas as pl
from jax.experimental.pallas import tpu as pltpu
from jax.sharding import PartitionSpec as P

ENTROPIC = 0.25
LANES = 128
SUBLANES = 8
CHUNKS = 16
CORES = 2
QUARTERS = 4
MESH = pl.DeviceIdType.MESH
SLOTS = range(16)
KX, RX, MX, CS, CB, A1, F0, AR, LS, B0, W1, F1, AX, BX, AO, BO = SLOTS


def eye():
    shape = (LANES, LANES)
    return lax.broadcasted_iota(jnp.int32, shape, 0) == lax.broadcasted_iota(jnp.int32, shape, 1)


def total(x):
    return jnp.sum(jnp.sum(x, axis=0, keepdims=True), axis=1, keepdims=True)


def tree(values):
    while len(values) > 1:
        values = [a + b for a, b in zip(values[::2], values[1::2])] + values[len(values) // 2 * 2 :]
    return values[0]


def signal(sem, target):
    pl.semaphore_signal(sem, inc=1, device_id={"chain": target}, device_id_type=MESH)


def chain_kernel(
    width, kernels, cost, marginals, final, out,
    kernel, column, marg, fin, row_out, row_in, rsum, col_out, col_in, cs_in, many,
    a1_in, f_out, f0_in, f1_in, ar_in, b0_out, b0_in, w0, w1_out, w1_in,
    alpha, alpha_in, beta, beta_in, alpha_last, beta_last,
    load_sem, send_sem, recv_sem, token,
):
    states = kernel.shape[1]
    rows = kernel.shape[0] // CORES
    blocks = states // LANES
    piece = kernel.shape[0] // LANES
    own = piece // CORES
    chips = width // CORES
    me = lax.axis_index("chain")
    g = me // width
    m = me % width
    chip = m // CORES
    core = m % CORES
    mate = me + 1 - 2 * core
    start = g * width
    first_g, last_g = g == 0, g == kernels - 1
    lead = core == 1
    up_collector = jnp.logical_and(lead, chip == chips - 1)
    down_collector = jnp.logical_and(lead, chip == 0)
    owner = start + width - 1

    def when(condition):
        return pl.when(condition)

    def both(*conditions):
        return functools.reduce(jnp.logical_and, conditions)

    def no(condition):
        return jnp.logical_not(condition)

    def copy(src, dst, slot, target):
        return pltpu.make_async_remote_copy(
            src_ref=src, dst_ref=dst, send_sem=send_sem.at[slot], recv_sem=recv_sem.at[slot],
            device_id={"chain": target}, device_id_type=MESH,
        )

    def received(ref, slot):
        copy(ref, ref, slot, mate).wait_recv()

    def sent(ref, slot):
        copy(ref, ref, slot, mate).wait_send()

    span = rows // CHUNKS
    base = core * rows

    def load(c):
        return pltpu.make_async_copy(
            cost.at[pl.ds(c * span, span)], kernel.at[pl.ds(base + c * span, span)], load_sem.at[c]
        )

    for c in range(CHUNKS):
        load(c).start()
    marg_load = pltpu.make_async_copy(marginals, marg.at[core], load_sem.at[CHUNKS])
    fin_load = pltpu.make_async_copy(final, fin, load_sem.at[CHUNKS + 1])
    marg_load.start()
    fin_load.start()

    barrier = pltpu.get_barrier_semaphore()
    signal(barrier, mate)

    @when(both(me != owner, mate != owner))
    def _():
        signal(barrier, owner)

    @when(both(me != start + 1, mate != start + 1))
    def _():
        signal(barrier, start + 1)

    @when(no(first_g))
    def _():
        signal(barrier, owner - width)

    @when(no(last_g))
    def _():
        signal(barrier, start + width + 1)

    @when(up_collector)
    def _():
        for i in range(width - CORES):
            if i != 1:
                signal(barrier, start + i)

    def lanes(b):
        return slice(b * LANES, (b + 1) * LANES)

    def row_of_column(ref, first, count):
        parts = []
        for h in range(first, first + count):
            x = jnp.sum(ref[h * LANES : (h + 1) * LANES, :], axis=1, keepdims=True)
            parts.append(jnp.sum(jnp.where(eye(), x, 0.0), axis=0, keepdims=True))
        return jnp.concatenate(parts, axis=0)

    def column_of_row(value):
        for h in range(piece):
            x = jnp.broadcast_to(value[h : h + 1, :], (LANES, LANES))
            x = jnp.sum(jnp.where(eye(), x, 0.0), axis=1, keepdims=True)
            column[h * LANES : (h + 1) * LANES, :] = jnp.broadcast_to(x, (LANES, LANES))

    def forward(v, order, send):
        column_of_row(v)
        row = jnp.sum(v * rsum[...], axis=0, keepdims=True)
        quarters = min(QUARTERS, chips)
        for q in range(quarters):
            targets = order[q * chips // quarters : (q + 1) * chips // quarters]
            mine = [i * piece + h for i in targets for h in range(piece)]

            def step(r, acc):
                at = pl.ds(pl.multiple_of(r * SUBLANES, SUBLANES), SUBLANES)
                v = column[at, :]
                return tuple(a + kernel[at, lanes(b)] * v for a, b in zip(acc, mine))

            zero = tuple(jnp.zeros((SUBLANES, LANES), jnp.float32) for _ in mine)
            acc = lax.fori_loop(0, CORES * rows // SUBLANES, step, zero, unroll=16)
            for n, i in enumerate(targets):
                for h in range(piece):
                    f_out[i, h : h + 1, :] = jnp.sum(acc[n * piece + h], axis=0, keepdims=True)
                f_out[i, piece : piece + 1, :] = row
            for i in targets:
                send(i)

    def backward(w, emit):
        ws = [jnp.broadcast_to(w(b), (SUBLANES, LANES)) for b in range(blocks)]

        def step(r, carry):
            at = pl.ds(pl.multiple_of(r * SUBLANES, SUBLANES), SUBLANES)
            x = [kernel[at, lanes(b)] * ws[b] for b in range(4)]
            for b in range(4, blocks):
                x[b % 4] = x[b % 4] + kernel[at, lanes(b)] * ws[b]
            column[at, :] = tree(x)
            return carry

        for h in range(CORES):
            lax.fori_loop(h * rows // SUBLANES, (h + 1) * rows // SUBLANES, step, 0, unroll=8)
            emit(h, row_of_column(column, h * own, own))

    def sum_pieces(ref):
        x = tree([ref[i] for i in range(chips)])
        return x[:piece], total(x[piece:])

    rate = -math.log2(math.e) / ENTROPIC

    def chunk_step(r, acc):
        at = pl.ds(pl.multiple_of(base + r * SUBLANES, SUBLANES), SUBLANES)
        new, xs = [], []
        for b in range(blocks):
            x = jnp.exp2(kernel[at, lanes(b)] * rate)
            kernel[at, lanes(b)] = x
            xs.append(x)
            new.append(acc[b] + x)
        here = pl.ds(pl.multiple_of(r * SUBLANES, SUBLANES), SUBLANES)
        column[here, :] = tree(xs)
        return tuple(new)

    acc = tuple(jnp.zeros((SUBLANES, LANES), jnp.float32) for _ in range(blocks))
    for c in range(CHUNKS):
        load(c).wait()
        acc = lax.fori_loop(c * span // SUBLANES, (c + 1) * span // SUBLANES, chunk_step, acc)
    for b in range(blocks):
        col_out[b // piece, b % piece : b % piece + 1, :] = jnp.sum(acc[b], axis=0, keepdims=True)

    greeted = jnp.where(mate == owner, 1, 2)
    greeted = jnp.where(down_collector, width - 1 + jnp.where(first_g, 0, width), greeted)
    greeted = jnp.where(up_collector, width - 1 + jnp.where(last_g, 0, width), greeted)
    pl.semaphore_wait(barrier, greeted)

    UP, DOWN = 0, 1

    @when(both(up_collector, no(last_g)))
    def _():
        for i in range(width - 1):
            signal(token.at[UP], start + i)

    @when(both(down_collector, no(first_g)))
    def _():
        for i in range(width):
            if i != 1:
                signal(token.at[DOWN], start + i)

    @when(no(up_collector))
    def _():
        copy(col_out, cs_in.at[m], CS, owner).start()

    row_out[...] = row_of_column(column, 0, own)
    marg_load.wait()
    fin_load.wait()
    copy(row_out, row_in, RX, mate).start()
    copy(marg.at[core], marg.at[core], MX, mate).start()
    half = kernel.at[pl.ds(base, rows)]
    copy(half, half, KX, mate).start()

    def wait_up():
        @when(both(no(up_collector), no(last_g)))
        def _():
            pl.semaphore_wait(token.at[UP], 1)

    def wait_down():
        @when(both(no(down_collector), no(first_g)))
        def _():
            pl.semaphore_wait(token.at[DOWN], 1)

    def to_group(src, dst, slot, group, i):
        copy(src, dst.at[chip], slot, group * width + CORES * i + core).start()

    high = list(range(chips - 1, -1, -1))
    low = list(range(chips))

    @when(up_collector)
    def _():
        cs_in[width - 1] = col_out[...]
        received(cs_in.at[pl.ds(0, width - 1)], CS)
        c = tree([cs_in[i] for i in range(width)])
        col_in[...] = c

        @when(first_g)
        def _():
            w0[...] = c * (states / total(jnp.sum(c, axis=0)))
            for i in high:
                copy(w0.at[i], a1_in, A1, start + width + CORES * i + 1).start()

        for i in range(width - 1):
            copy(col_in, col_in, CB, start + i).start()

    received(row_in, RX)

    @when(lead)
    def _():
        rsum[...] = jnp.concatenate([row_in[...], row_out[...]], axis=0)

    @when(no(lead))
    def _():
        rsum[...] = jnp.concatenate([row_out[...], row_in[...]], axis=0)

    received(marg.at[1 - core], MX)
    target = jnp.concatenate([marg[i] for i in range(CORES)], axis=0)

    def factor(products):
        return states / total(jnp.sum(products, axis=0))

    @when(lead)
    def _():
        alpha[...] = jnp.ones_like(alpha)

        @when(g == 1)
        def _():
            received(a1_in, A1)
            alpha[...] = a1_in[...]

        @when(g > 1)
        def _():
            received(f0_in, F0)
            a, s = sum_pieces(f0_in)
            alpha[...] = a * (states / s)

        received(kernel.at[pl.ds(0, rows)], KX)
        wait_up()

        @when(no(first_g))
        def _():
            def send(i):
                @when(no(last_g))
                def _():
                    to_group(f_out.at[i], f0_in, F0, g + 1, i)

                @when(both(last_g, no(up_collector)))
                def _():
                    copy(f_out.at[i, pl.ds(0, piece)], ar_in.at[chip, i], AR, owner).start()

            forward(alpha[...], high, send)
            copy(alpha, alpha_in, AX, mate).start()

        @when(both(last_g, no(up_collector)))
        def _():
            received(w1_in, LS)

        @when(both(last_g, up_collector))
        def _():
            ar_in[chips - 1] = f_out[:, :piece, :]
            received(ar_in.at[pl.ds(0, chips - 1)], AR)
            x = tree([ar_in[i] for i in range(chips)])
            x = fin[...] / (x * (states / total(jnp.sum(x, axis=0))))
            for h in range(CORES):
                w1_in[h] = x[:, h * own : (h + 1) * own]
            for i in range(chips - 1):
                copy(w1_in, w1_in, LS, start + CORES * i + 1).start()

        @when(no(up_collector))
        def _():
            received(col_in, CB)

        received(beta_in, BX)
        scaling = target / (alpha[...] * beta_in[...])

        @when(no(last_g))
        def _():
            received(w1_in, W1)

        wait_down()

        def send_w(h, b):
            f = factor(sum(col_in[:, k * own : (k + 1) * own, :] * w1_in[k] for k in range(CORES)))
            b = b * f
            beta_last[h] = b
            if h == 0:
                copy(beta_last.at[0], beta_last.at[0], BO, mate).start()

            @when(no(first_g))
            def _():
                w1_out[h, 0] = scaling[h * own : (h + 1) * own] * b
                for i in low:
                    copy(w1_out.at[h, 0], w1_in.at[h, chip], W1, start - width + CORES * i + core).start()

        backward(lambda b: w1_in[b % piece // own, b // piece, b % own : b % own + 1, :], send_w)
        received(alpha_last, AO)
        out[...] = target[own:] / (alpha_last[own:, :] * beta_last[1])

    @when(no(lead))
    def _():
        def send_b(b):
            b0_out[0:piece, :] = b
            b0_out[piece : piece + 1, :] = jnp.sum(b, axis=0, keepdims=True)
            wait_down()
            for i in low:
                to_group(b0_out, b0_in, B0, g - 1, i)

        @when(last_g)
        def _():
            send_b(rsum[...])
            received(col_in, CB)
            beta[...] = rsum[...] * factor(col_in[...])

        received(kernel.at[pl.ds(rows, rows)], KX)

        @when(no(last_g))
        def _():
            received(b0_in, B0)
            x = b0_in[...]
            s = total(tree([x[i, piece:] for i in range(chips)]))
            w0[...] = x[:, :piece] * (states / s)

            def keep(h, b):
                beta[h * own : (h + 1) * own, :] = b

            backward(lambda b: w0[b // piece, b % piece : b % piece + 1, :], keep)

            @when(no(first_g))
            def _():
                send_b(beta[...])

            received(col_in, CB)
            beta[...] = beta[...] * factor(col_in[...] * w0[...])

        copy(beta, beta_in, BX, mate).start()
        alpha_last[...] = jnp.ones_like(alpha_last)
        alpha_in_value = jnp.ones((piece, LANES), jnp.float32)

        @when(first_g)
        def _():
            alpha_in[...] = alpha_in_value

        @when(no(first_g))
        def _():
            received(alpha_in, AX)
            received(f1_in, F1)
            a, s = sum_pieces(f1_in)
            alpha_last[...] = a * (states / s)

        copy(alpha_last, alpha_last, AO, mate).start()
        wait_up()

        @when(no(last_g))
        def _():
            scaling = target / (alpha_in[...] * beta[...])
            forward(scaling * alpha_last[...], high, lambda i: to_group(f_out.at[i], f1_in, F1, g + 1, i))

        received(beta_last.at[0], BO)
        out[...] = target[:own] / (alpha_last[:own, :] * beta_last[0])

    sent(row_in, RX)
    sent(marg.at[core], MX)
    sent(half, KX)

    @when(no(up_collector))
    def _():
        sent(col_out, CS)

    @when(lead)
    def _():
        sent(beta_last.at[0], BO)

        @when(up_collector)
        def _():
            sent(many, CB)

            @when(first_g)
            def _():
                sent(col_in, A1)

        @when(both(g > 0, no(last_g)))
        def _():
            sent(f0_in, F0)

        @when(no(first_g))
        def _():
            sent(alpha, AX)
            sent(w1_in, W1)

        @when(both(last_g, no(up_collector)))
        def _():
            sent(w0, AR)

        @when(both(last_g, up_collector))
        def _():
            sent(many.at[pl.ds(0, chips - 1)], LS)

    @when(no(lead))
    def _():
        sent(beta, BX)
        sent(alpha_last, AO)

        @when(no(first_g))
        def _():
            sent(b0_in, B0)

        @when(no(last_g))
        def _():
            sent(f1_in, F1)


def solution(mesh):
    chain = mesh.shape["chain"]

    def on_device(cost, marginals, final_marginal):
        rows, states = cost.shape
        width = states // rows
        chips = width // CORES
        own = rows // LANES
        piece = CORES * own

        def buffer(*shape):
            return pltpu.VMEM(shape + (LANES,), jnp.float32)

        one = buffer(piece)
        whole = buffer(chips, piece)
        pieces = buffer(chips, piece + 1)
        scratch = dict(
            kernel=pltpu.VMEM((CORES * rows, states), jnp.float32), column=buffer(CORES * rows),
            marg=buffer(CORES, own), fin=whole, row_out=buffer(own), row_in=buffer(own), rsum=one,
            col_out=whole, col_in=whole, cs_in=buffer(width, chips, piece),
            many=buffer(width - 1, chips, piece),
            a1_in=one, f_out=pieces, f0_in=pieces, f1_in=pieces, ar_in=buffer(chips, chips, piece),
            b0_out=buffer(piece + 1), b0_in=pieces, w0=whole, w1_out=buffer(CORES, chips, own), w1_in=buffer(CORES, chips, own),
            alpha=one, alpha_in=one, beta=one, beta_in=one, alpha_last=one, beta_last=buffer(CORES, own),
            load_sem=pltpu.SemaphoreType.DMA((CHUNKS + 2,)), send_sem=pltpu.SemaphoreType.DMA((len(SLOTS),)),
            recv_sem=pltpu.SemaphoreType.DMA((len(SLOTS),)), token=pltpu.SemaphoreType.REGULAR((2,)),
        )
        scaling = pl.pallas_call(
            functools.partial(chain_kernel, width, chain // width),
            out_shape=pltpu.VMEM((own, LANES), jnp.float32),
            in_specs=[pl.BlockSpec(memory_space=pl.ANY)] * 3,
            out_specs=pl.BlockSpec(memory_space=pltpu.VMEM),
            scratch_shapes=scratch,
            compiler_params=pltpu.CompilerParams(collective_id=0, has_side_effects=True),
            name="sinkhorn_chain",
        )(cost, marginals.reshape(own, LANES), final_marginal.reshape(chips, piece, LANES))
        return jnp.log(scaling).reshape(rows)

    placed = (P(("pop", "chain"), None), P(("pop", "chain")), P("pop"))
    return jax.shard_map(on_device, mesh=mesh, in_specs=placed, out_specs=P(("pop", "chain")), check_vma=False)
```

```python
import functools
import math

import jax
import jax.numpy as jnp
from jax import lax
from jax.experimental import pallas as pl
from jax.experimental.pallas import tpu as pltpu
from jax.sharding import PartitionSpec as P

ENTROPIC = 0.25
LANES = 128
SUBLANES = 8
CHUNKS = 16
CORES = 2
QUARTERS = 4
OWNERS = 2
MESH = pl.DeviceIdType.MESH
SLOTS = range(16)
KX, RX, MX, CS, CB, A1, F0, AR, LS, B0, W1, F1, AX, BX, AO, BO = SLOTS


def eye():
    shape = (LANES, LANES)
    return lax.broadcasted_iota(jnp.int32, shape, 0) == lax.broadcasted_iota(jnp.int32, shape, 1)


def total(x):
    return jnp.sum(jnp.sum(x, axis=0, keepdims=True), axis=1, keepdims=True)


def tree(values):
    while len(values) > 1:
        values = [a + b for a, b in zip(values[::2], values[1::2])] + values[len(values) // 2 * 2 :]
    return values[0]


def signal(sem, target):
    pl.semaphore_signal(sem, inc=1, device_id={"chain": target}, device_id_type=MESH)


def chain_kernel(
    width, kernels, cost, marginals, final, out,
    kernel, column, marg, fin, row_out, row_in, rsum, col_out, col_in, cs_in, many,
    a1_in, f_out, f0_in, f1_in, ar_in, b0_out, b0_in, w0, w1_out, w1_in,
    alpha, alpha_in, beta, beta_in, alpha_last, beta_last,
    load_sem, send_sem, recv_sem, token,
):
    states = kernel.shape[1]
    rows = kernel.shape[0] // CORES
    blocks = states // LANES
    piece = kernel.shape[0] // LANES
    own = piece // CORES
    chips = width // CORES
    me = lax.axis_index("chain")
    g = me // width
    m = me % width
    chip = m // CORES
    core = m % CORES
    mate = me + 1 - 2 * core
    start = g * width
    first_g, last_g = g == 0, g == kernels - 1
    lead = core == 1
    up_collector = jnp.logical_and(lead, chip == chips - 1)
    down_collector = jnp.logical_and(lead, chip == 0)
    owner = start + width - 1
    share = chips // OWNERS

    def when(condition):
        return pl.when(condition)

    def both(*conditions):
        return functools.reduce(jnp.logical_and, conditions)

    def no(condition):
        return jnp.logical_not(condition)

    def copy(src, dst, slot, target):
        return pltpu.make_async_remote_copy(
            src_ref=src, dst_ref=dst, send_sem=send_sem.at[slot], recv_sem=recv_sem.at[slot],
            device_id={"chain": target}, device_id_type=MESH,
        )

    def received(ref, slot):
        copy(ref, ref, slot, mate).wait_recv()

    def sent(ref, slot):
        copy(ref, ref, slot, mate).wait_send()

    span = rows // CHUNKS
    base = core * rows

    def load(c):
        return pltpu.make_async_copy(
            cost.at[pl.ds(c * span, span)], kernel.at[pl.ds(base + c * span, span)], load_sem.at[c]
        )

    for c in range(CHUNKS):
        load(c).start()
    marg_load = pltpu.make_async_copy(marginals, marg.at[core], load_sem.at[CHUNKS])
    fin_load = pltpu.make_async_copy(final, fin, load_sem.at[CHUNKS + 1])
    marg_load.start()
    fin_load.start()

    barrier = pltpu.get_barrier_semaphore()
    signal(barrier, mate)

    @when(both(me != owner, mate != owner))
    def _():
        signal(barrier, owner)

    @when(both(me != start + 1, mate != start + 1))
    def _():
        signal(barrier, start + 1)

    @when(no(first_g))
    def _():
        signal(barrier, owner - width)

    @when(no(last_g))
    def _():
        signal(barrier, start + width + 1)

    @when(up_collector)
    def _():
        for i in range(width - CORES):
            if i != 1:
                signal(barrier, start + i)

    def lanes(b):
        return slice(b * LANES, (b + 1) * LANES)

    def row_of_column(ref, first, count):
        parts = []
        for h in range(first, first + count):
            x = jnp.sum(ref[h * LANES : (h + 1) * LANES, :], axis=1, keepdims=True)
            parts.append(jnp.sum(jnp.where(eye(), x, 0.0), axis=0, keepdims=True))
        return jnp.concatenate(parts, axis=0)

    def column_of_row(value):
        for h in range(piece):
            x = jnp.broadcast_to(value[h : h + 1, :], (LANES, LANES))
            x = jnp.sum(jnp.where(eye(), x, 0.0), axis=1, keepdims=True)
            column[h * LANES : (h + 1) * LANES, :] = jnp.broadcast_to(x, (LANES, LANES))

    def forward(v, order, send):
        column_of_row(v)
        row = jnp.sum(v * rsum[...], axis=0, keepdims=True)
        quarters = min(QUARTERS, chips)
        for q in range(quarters):
            targets = order[q * chips // quarters : (q + 1) * chips // quarters]
            mine = [i * piece + h for i in targets for h in range(piece)]

            def step(r, acc):
                at = pl.ds(pl.multiple_of(r * SUBLANES, SUBLANES), SUBLANES)
                v = column[at, :]
                return tuple(a + kernel[at, lanes(b)] * v for a, b in zip(acc, mine))

            zero = tuple(jnp.zeros((SUBLANES, LANES), jnp.float32) for _ in mine)
            acc = lax.fori_loop(0, CORES * rows // SUBLANES, step, zero, unroll=16)
            for n, i in enumerate(targets):
                for h in range(piece):
                    f_out[i, h : h + 1, :] = jnp.sum(acc[n * piece + h], axis=0, keepdims=True)
                f_out[i, piece : piece + 1, :] = row
            for i in targets:
                send(i)

    def backward(w, emit):
        ws = [jnp.broadcast_to(w(b), (SUBLANES, LANES)) for b in range(blocks)]

        def step(r, carry):
            at = pl.ds(pl.multiple_of(r * SUBLANES, SUBLANES), SUBLANES)
            x = [kernel[at, lanes(b)] * ws[b] for b in range(4)]
            for b in range(4, blocks):
                x[b % 4] = x[b % 4] + kernel[at, lanes(b)] * ws[b]
            column[at, :] = tree(x)
            return carry

        for h in range(CORES):
            lax.fori_loop(h * rows // SUBLANES, (h + 1) * rows // SUBLANES, step, 0, unroll=8)
            emit(h, row_of_column(column, h * own, own))

    def sum_pieces(ref):
        x = tree([ref[i] for i in range(chips)])
        return x[:piece], total(x[piece:])

    rate = -math.log2(math.e) / ENTROPIC

    def chunk_step(r, acc):
        at = pl.ds(pl.multiple_of(base + r * SUBLANES, SUBLANES), SUBLANES)
        new, xs = [], []
        for b in range(blocks):
            x = jnp.exp2(kernel[at, lanes(b)] * rate)
            kernel[at, lanes(b)] = x
            xs.append(x)
            new.append(acc[b] + x)
        here = pl.ds(pl.multiple_of(r * SUBLANES, SUBLANES), SUBLANES)
        column[here, :] = tree(xs)
        return tuple(new)

    acc = tuple(jnp.zeros((SUBLANES, LANES), jnp.float32) for _ in range(blocks))
    for c in range(CHUNKS):
        load(c).wait()
        acc = lax.fori_loop(c * span // SUBLANES, (c + 1) * span // SUBLANES, chunk_step, acc)
    for b in range(blocks):
        col_out[b // piece, b % piece : b % piece + 1, :] = jnp.sum(acc[b], axis=0, keepdims=True)

    greeted = jnp.where(mate == owner, 1, 2)
    greeted = jnp.where(down_collector, width - 1 + jnp.where(first_g, 0, width), greeted)
    greeted = jnp.where(up_collector, width - 1 + jnp.where(last_g, 0, width), greeted)
    pl.semaphore_wait(barrier, greeted)

    UP, DOWN = 0, 1

    @when(both(up_collector, no(last_g)))
    def _():
        for i in range(width - 1):
            signal(token.at[UP], start + i)

    @when(both(down_collector, no(first_g)))
    def _():
        for i in range(width):
            if i != 1:
                signal(token.at[DOWN], start + i)

    @when(no(up_collector))
    def _():
        copy(col_out, cs_in.at[m], CS, owner).start()

    row_out[...] = row_of_column(column, 0, own)
    marg_load.wait()
    fin_load.wait()
    copy(row_out, row_in, RX, mate).start()
    copy(marg.at[core], marg.at[core], MX, mate).start()
    half = kernel.at[pl.ds(base, rows)]
    copy(half, half, KX, mate).start()

    def wait_up():
        @when(both(no(up_collector), no(last_g)))
        def _():
            pl.semaphore_wait(token.at[UP], 1)

    def wait_down():
        @when(both(no(down_collector), no(first_g)))
        def _():
            pl.semaphore_wait(token.at[DOWN], 1)

    def to_group(src, dst, slot, group, i):
        copy(src, dst.at[chip], slot, group * width + CORES * i + core).start()

    high = list(range(chips - 1, -1, -1))
    low = list(range(chips))

    @when(up_collector)
    def _():
        cs_in[width - 1] = col_out[...]
        received(cs_in.at[pl.ds(0, width - 1)], CS)
        c = tree([cs_in[i] for i in range(width)])
        col_in[...] = c

        @when(first_g)
        def _():
            w0[...] = c * (states / total(jnp.sum(c, axis=0)))
            for i in high:
                copy(w0.at[i], a1_in, A1, start + width + CORES * i + 1).start()

        for i in range(width - 1):
            copy(col_in, col_in, CB, start + i).start()

    received(row_in, RX)

    @when(lead)
    def _():
        rsum[...] = jnp.concatenate([row_in[...], row_out[...]], axis=0)

    @when(no(lead))
    def _():
        rsum[...] = jnp.concatenate([row_out[...], row_in[...]], axis=0)

    received(marg.at[1 - core], MX)
    target = jnp.concatenate([marg[i] for i in range(CORES)], axis=0)

    def factor(products):
        return states / total(jnp.sum(products, axis=0))

    @when(lead)
    def _():
        alpha[...] = jnp.ones_like(alpha)

        @when(g == 1)
        def _():
            received(a1_in, A1)
            alpha[...] = a1_in[...]

        @when(g > 1)
        def _():
            received(f0_in, F0)
            a, s = sum_pieces(f0_in)
            alpha[...] = a * (states / s)

        received(kernel.at[pl.ds(0, rows)], KX)
        wait_up()
        wait_down()

        @when(no(first_g))
        def _():
            def send(i):
                @when(no(last_g))
                def _():
                    to_group(f_out.at[i], f0_in, F0, g + 1, i)

                taker = chips - OWNERS + i // share

                @when(both(last_g, chip != taker))
                def _():
                    copy(f_out.at[i], ar_in.at[chip, i % share], AR, start + CORES * taker + 1).start()

            forward(alpha[...], high, send)
            copy(alpha, alpha_in, AX, mate).start()

        for o in range(OWNERS):
            taker = chips - OWNERS + o
            part = pl.ds(o * share, share)

            @when(both(last_g, chip == taker))
            def _():
                ar_in[taker] = f_out[part]
                received(ar_in.at[pl.ds(0, chips - 1)], AR)
                x = tree([ar_in[i] for i in range(chips)])
                x = fin[part] / (x[:, :piece] * (states / total(x[0, piece:])))
                for h in range(CORES):
                    w1_in[h, part] = x[:, h * own : (h + 1) * own]
                for i in range(chips):
                    for h in range(CORES):
                        if i != taker:
                            copy(w1_in.at[h, part], w1_in.at[h, part], LS, start + CORES * i + 1).start()
                received(w1_in.at[0], LS)

        @when(both(last_g, chip < chips - OWNERS))
        def _():
            received(w1_in, LS)

        @when(no(up_collector))
        def _():
            received(col_in, CB)

        received(beta_in, BX)
        scaling = target / (alpha[...] * beta_in[...])

        @when(no(last_g))
        def _():
            received(w1_in, W1)

        def send_w(h, b):
            f = factor(sum(col_in[:, k * own : (k + 1) * own, :] * w1_in[k] for k in range(CORES)))
            b = b * f
            beta_last[h] = b
            if h == 0:
                copy(beta_last.at[0], beta_last.at[0], BO, mate).start()

            @when(no(first_g))
            def _():
                w1_out[h, 0] = scaling[h * own : (h + 1) * own] * b
                for i in low:
                    copy(w1_out.at[h, 0], w1_in.at[h, chip], W1, start - width + CORES * i + core).start()

        backward(lambda b: w1_in[b % piece // own, b // piece, b % own : b % own + 1, :], send_w)
        received(alpha_last, AO)
        out[...] = target[own:] / (alpha_last[own:, :] * beta_last[1])

    @when(no(lead))
    def _():
        def send_b(b):
            b0_out[0:piece, :] = b
            b0_out[piece : piece + 1, :] = jnp.sum(b, axis=0, keepdims=True)
            wait_down()
            for i in low:
                to_group(b0_out, b0_in, B0, g - 1, i)

        @when(last_g)
        def _():
            send_b(rsum[...])
            received(col_in, CB)
            beta[...] = rsum[...] * factor(col_in[...])

        received(kernel.at[pl.ds(rows, rows)], KX)

        @when(no(last_g))
        def _():
            received(b0_in, B0)
            x = b0_in[...]
            s = total(tree([x[i, piece:] for i in range(chips)]))
            w0[...] = x[:, :piece] * (states / s)

            def keep(h, b):
                beta[h * own : (h + 1) * own, :] = b

            backward(lambda b: w0[b // piece, b % piece : b % piece + 1, :], keep)

            @when(no(first_g))
            def _():
                send_b(beta[...])

            received(col_in, CB)
            beta[...] = beta[...] * factor(col_in[...] * w0[...])

        copy(beta, beta_in, BX, mate).start()
        alpha_last[...] = jnp.ones_like(alpha_last)
        alpha_in_value = jnp.ones((piece, LANES), jnp.float32)

        @when(first_g)
        def _():
            alpha_in[...] = alpha_in_value

        @when(no(first_g))
        def _():
            received(alpha_in, AX)
            received(f1_in, F1)
            a, s = sum_pieces(f1_in)
            alpha_last[...] = a * (states / s)

        copy(alpha_last, alpha_last, AO, mate).start()
        wait_up()

        @when(no(last_g))
        def _():
            scaling = target / (alpha_in[...] * beta[...])
            forward(scaling * alpha_last[...], high, lambda i: to_group(f_out.at[i], f1_in, F1, g + 1, i))

        received(beta_last.at[0], BO)
        out[...] = target[:own] / (alpha_last[:own, :] * beta_last[0])

    sent(row_in, RX)
    sent(marg.at[core], MX)
    sent(half, KX)

    @when(no(up_collector))
    def _():
        sent(col_out, CS)

    @when(lead)
    def _():
        sent(beta_last.at[0], BO)

        @when(up_collector)
        def _():
            sent(many, CB)

            @when(first_g)
            def _():
                sent(col_in, A1)

        @when(both(g > 0, no(last_g)))
        def _():
            sent(f0_in, F0)

        @when(no(first_g))
        def _():
            sent(alpha, AX)
            sent(w1_in, W1)

        @when(both(last_g, chip < chips - OWNERS))
        def _():
            sent(f_out, AR)

        @when(both(last_g, chip >= chips - OWNERS))
        def _():
            sent(f_out.at[pl.ds(0, share)], AR)
            sent(many.at[pl.ds(0, chips - 1), pl.ds(0, share)], LS)

    @when(no(lead))
    def _():
        sent(beta, BX)
        sent(alpha_last, AO)

        @when(no(first_g))
        def _():
            sent(b0_in, B0)

        @when(no(last_g))
        def _():
            sent(f1_in, F1)


def solution(mesh):
    chain = mesh.shape["chain"]

    def on_device(cost, marginals, final_marginal):
        rows, states = cost.shape
        width = states // rows
        chips = width // CORES
        own = rows // LANES
        piece = CORES * own

        def buffer(*shape):
            return pltpu.VMEM(shape + (LANES,), jnp.float32)

        one = buffer(piece)
        whole = buffer(chips, piece)
        pieces = buffer(chips, piece + 1)
        scratch = dict(
            kernel=pltpu.VMEM((CORES * rows, states), jnp.float32), column=buffer(CORES * rows),
            marg=buffer(CORES, own), fin=whole, row_out=buffer(own), row_in=buffer(own), rsum=one,
            col_out=whole, col_in=whole, cs_in=buffer(width, chips, piece),
            many=buffer(width - 1, chips, piece),
            a1_in=one, f_out=pieces, f0_in=pieces, f1_in=pieces, ar_in=buffer(chips, chips // OWNERS, piece + 1),
            b0_out=buffer(piece + 1), b0_in=pieces, w0=whole, w1_out=buffer(CORES, chips, own), w1_in=buffer(CORES, chips, own),
            alpha=one, alpha_in=one, beta=one, beta_in=one, alpha_last=one, beta_last=buffer(CORES, own),
            load_sem=pltpu.SemaphoreType.DMA((CHUNKS + 2,)), send_sem=pltpu.SemaphoreType.DMA((len(SLOTS),)),
            recv_sem=pltpu.SemaphoreType.DMA((len(SLOTS),)), token=pltpu.SemaphoreType.REGULAR((2,)),
        )
        scaling = pl.pallas_call(
            functools.partial(chain_kernel, width, chain // width),
            out_shape=pltpu.VMEM((own, LANES), jnp.float32),
            in_specs=[pl.BlockSpec(memory_space=pl.ANY)] * 3,
            out_specs=pl.BlockSpec(memory_space=pltpu.VMEM),
            scratch_shapes=scratch,
            compiler_params=pltpu.CompilerParams(collective_id=0, has_side_effects=True),
            name="sinkhorn_chain",
        )(cost, marginals.reshape(own, LANES), final_marginal.reshape(chips, piece, LANES))
        return jnp.log(scaling).reshape(rows)

    placed = (P(("pop", "chain"), None), P(("pop", "chain")), P("pop"))
    return jax.shard_map(on_device, mesh=mesh, in_specs=placed, out_specs=P(("pop", "chain")), check_vma=False)
```
